32 devices in a mesh: dp: 8 (over z, y), tensor: 4 (over x, core).
Axes of the slice: x: 2, y: 2, z: 4, core: 2. Of those that a mesh axis runs over, the one named last changes fastest.
Arguments:
- out_grad: bfloat16 [2048, 1024], P('dp'), may hold values from -0.29882812 to 0.29882812
- hidden: bfloat16 [2048, 28672], P('dp', 'tensor'), may hold values from -60 to 60
- momentum: float32 [1024, 28672], P('dp', 'tensor'), may hold values from -48 to 48
- second: float32 [1024], P('dp'), may hold values from 0.01 to 0.2
Outputs:
- update: bfloat16 [1024, 28672], P('dp', 'tensor')
- momentum_out: float32 [1024, 28672], P('dp', 'tensor')
- second_out: float32 [1024], P('dp')
The draws below stay inside these ranges and needn't reach their ends.
All inputs are finite; a program needn't handle non-finite values.
Results may differ from the reference program's by a relative error of at most 0.035.
Values may be sent and summed in bfloat16 or wider, within the bound.
A program may use at most 128 MiB of HBM per device.

```python
import math
import jax
import jax.numpy as jnp
from jax import lax

FF = 28672
ROWS_DEV = 128
ITERS = 3
ROWS = 1024
TOKENS = 2048
N_DP = 8


def draw_hidden(key, part):
    first_key = jax.random.fold_in(jax.random.fold_in(key, 17), 0)
    column_ramp = jnp.exp(jnp.log(3.0) * jnp.arange(FF, dtype=jnp.float32) / FF)
    base_values = jnp.clip(jax.random.normal(first_key, (TOKENS, FF), jnp.float32), -6.0, 6.0)
    return (base_values * column_ramp[None, :]).astype(jnp.bfloat16)


def with_spikes(drawn, stream_key, source, target, blocks, factor):
    owner, partner = [(jnp.arange(drawn.shape[position]) // (drawn.shape[position] // blocks)).reshape([-1 if axis == position else 1 for axis in range(drawn.ndim)]) for position in (source, target)]
    chosen = jax.random.permutation(stream_key, blocks)[partner]
    strong = (owner == chosen) | (owner == (partner + blocks // 2) % blocks)
    return jnp.where(strong, factor * drawn, drawn)


def shard_levels(own_key, dims, cuts, low, top_value):
    factor_of, own = 1.0, jax.random.fold_in(own_key, 6)
    for dim, shards_of in cuts:
        heights = jnp.exp(jax.random.uniform(jax.random.fold_in(own, dim), (shards_of,), jnp.float32, low / len(cuts), top_value / len(cuts)))
        factor_of = factor_of * jnp.repeat(heights, dims[dim] // shards_of).reshape([-1 if axis == dim else 1 for axis in range(len(dims))])
    return factor_of


def normal_values(rng, dims, width, limit, cuts=(), held_as=jnp.bfloat16):
    array = jax.random.normal(rng, dims, jnp.float32) * width
    if len(cuts) > 0:
        array = shard_levels(rng, dims, cuts, -0.22, 0.18) * array
    return jnp.clip(array, min=-limit, max=limit).astype(held_as)


def heavy_noise(stream_key, dims, width, bound, shards, heavy, kind=jnp.bfloat16):
    entries = width * jax.random.normal(stream_key, dims, jnp.float32)
    if shards:
        entries = entries * shard_levels(stream_key, dims, shards, -0.22, 0.18)
    return jnp.clip(with_spikes(entries, jax.random.fold_in(stream_key, 3), *heavy), -bound, bound).astype(kind)


def setup_inputs(seed: int = 0) -> dict:
    splits = jax.random.split(jax.random.key(seed), 5)
    out_grad = heavy_noise(splits[0], (TOKENS, ROWS), 0.05, 0.29882812, ((0, 8),), (0, 1, 8, 2.0))
    hidden = draw_hidden(jax.random.fold_in(splits[4], 71), 0)
    momentum = normal_values(splits[2], (ROWS, FF), 8.0, 48.0, ((0, 8), (1, 4)), jnp.float32)
    second = jnp.clip(jnp.exp(math.log(0.2) - 2.9957323 * jax.random.uniform(splits[3], (ROWS,), jnp.float32) ** shard_levels(splits[3], (ROWS,), ((0, 8),), -0.2, 0.2)), 0.01, 0.2)
    return dict(out_grad=out_grad, hidden=hidden, momentum=momentum, second=second)


quintic_a = 3.4445
quintic_b = -4.775
quintic_c = 2.0315
beta_one = 0.95
beta_two = 0.95

def orthogonal_panel(panel):
    norm_sum = jnp.sqrt(jnp.sum(panel * panel))
    current = (panel / (norm_sum + 1e-07)).astype(jnp.bfloat16)
    for iteration in range(ITERS):
        gram = jnp.dot(current, current.T, preferred_element_type=jnp.float32).astype(jnp.bfloat16)
        square = jnp.dot(gram, gram, preferred_element_type=jnp.float32)
        poly = (quintic_b * gram.astype(jnp.float32) + quintic_c * square).astype(jnp.bfloat16)
        current = (quintic_a * current.astype(jnp.float32) + jnp.dot(poly, current, preferred_element_type=jnp.float32)).astype(jnp.bfloat16)
    return current

def reference(out_grad, hidden, momentum, second):
    tok_block = out_grad.shape[0] // N_DP
    grad_blocks = out_grad.reshape(N_DP, tok_block, out_grad.shape[1])
    hidden_blocks = hidden.reshape(N_DP, tok_block, hidden.shape[1])

    def add_block(running, pair):
        grad_block, hidden_block = pair
        partial_term = lax.dot_general(grad_block, hidden_block, (((0,), (0,)), ((), ())), preferred_element_type=jnp.float32)
        rounded = lax.optimization_barrier(partial_term.astype(jnp.bfloat16))
        return (running + rounded.astype(jnp.float32), None)
    start_sum = jnp.zeros((out_grad.shape[1], hidden.shape[1]), jnp.float32)
    grad, unused = lax.scan(add_block, start_sum, (grad_blocks, hidden_blocks))
    momentum_out = beta_one * momentum + grad
    nesterov = grad + beta_one * momentum_out
    panels = nesterov.reshape(N_DP, ROWS_DEV, FF)
    orthogonal = lax.map(orthogonal_panel, panels).reshape(ROWS_DEV * N_DP, FF)
    ortho_wide = orthogonal.astype(jnp.float32)
    energy = lax.optimization_barrier(jnp.sum(ortho_wide * ortho_wide, axis=1))
    second_out = beta_two * second + (1.0 - beta_two) * energy
    update = (ortho_wide * jnp.sqrt(FF / second_out)[:, None]).astype(jnp.bfloat16)
    return (update, momentum_out, second_out)
```

```python
import functools

import jax
import jax.numpy as jnp
from jax import lax
from jax.experimental import pallas as pl
from jax.experimental.pallas import tpu as pltpu
from jax.sharding import PartitionSpec as P

ITERS = 3
quintic_a = 3.4445
quintic_b = -4.775
quintic_c = 2.0315
beta_one = 0.95
beta_two = 0.95

MESH = pl.DeviceIdType.MESH
F32 = jnp.float32
BF16 = jnp.bfloat16


def line_split(n_dp):
    ny = 1
    while ny * ny * 4 <= n_dp and n_dp % (ny * 2) == 0:
        ny *= 2
    return n_dp // ny, ny


def exact_dot(a, b):
    return jnp.dot(a, b, preferred_element_type=F32, precision=lax.Precision.HIGHEST)


def kernel(
    nz, ny, nt, n, ff,
    og_hbm, h_hbm, mom_hbm, sec_ref,
    x, mom, final_ref, secout_ref,
    h, ograw, og_t, recv, send, fin, acc, gram, norm, g_all,
    h_sem, og_sem, og_own, recv_sem, fin_sem, mom_sem,
    hy_send, end_send, fwd_send, og_send, ogx_send, ogc_send, s_send, g_send, g_recv,
):
    tokens, part = h_hbm.shape[0], h_hbm.shape[1] // ny
    rows, width = x.shape[1], x.shape[2]
    group = ny * rows
    tau = tokens // nt
    nx = nt // 2
    slots = 2 * ny
    half = nz // 2
    ahead, end_ahead, lag, fin_lag = 6, 3, 2, 2
    d = lax.axis_index("dp")
    t = lax.axis_index("tensor")
    z, y = d // ny, lax.rem(d, ny)
    tx, core = t // 2, lax.rem(t, 2)
    lower = z * 2 < nz
    zm = jnp.where(lower, z, nz - 1 - z)
    toward = jnp.where(lower, 1, -1)
    is_end = zm == 0

    def mirrored(jm):
        return jnp.where(lower, jm, nz - 1 - jm)

    def far_slot(j):
        return jnp.where(lower, j + 1, j)

    def near_slot(j):
        return jnp.where(lower, j, j + 1)

    def at(zz, yy):
        return (zz * ny + yy, t)

    def at_y(k):
        return at(z, lax.rem(y + k, ny))

    def at_t(tt):
        return (d, tt)

    def when(cond, fn):
        if isinstance(cond, bool):
            if cond:
                fn()
        else:
            pl.when(cond)(fn)

    def remote(src, dst, send_sem, recv_sem, device):
        pltpu.make_async_remote_copy(
            src, dst, send_sem, recv_sem, device_id=device, device_id_type=MESH
        ).start()

    def arrived(ref, sem):
        pltpu.make_async_copy(ref, ref, sem).wait()

    def block(i, size):
        return pl.ds(pl.multiple_of(i * size, size), size)

    def columns(p, c):
        return block(p * n + c, width)

    inner_z = 1 if half == 2 else zm
    z_end = jnp.where(lower, 0, nz - 1)

    barrier = pltpu.get_barrier_semaphore()

    def hello(device):
        pl.semaphore_signal(barrier, inc=1, device_id=device, device_id_type=MESH)

    for k in range(1, ny):
        hello(at_y(k))
    for k in range(1, nt):
        hello(at_t(lax.rem(t + k, nt)))

    @pl.when(is_end)
    def _():
        for k in range(ny):
            hello(at(z + toward, k))

    @pl.when(jnp.logical_not(is_end))
    def _():
        hello(at(z + toward, y))

        def ends():
            for k in range(ny):
                hello(at(z_end, k))

        def next_in():
            hello(at(z - toward, y))

        if half == 2:
            ends()
        else:
            pl.when(zm == 1)(ends)
            pl.when(zm > 1)(next_in)

    greeted = (ny - 1) + (nt - 1)
    pl.semaphore_wait(
        barrier,
        greeted + jnp.where(zm == 0, ny, 0) + jnp.where(zm == 1, ny + 1, 0) + jnp.where(zm > 1, 2, 0),
    )

    piece = block(t, tau)

    def rows_of(j):
        return block(j, group)

    def y_send(c):
        for k in range(1, ny):
            p = lax.rem(y + k, ny)
            remote(
                h_hbm.at[:, columns(p, c)], h.at[c, block(y, tokens)],
                hy_send.at[k - 1], h_sem.at[y, c], at_y(k),
            )

    def mom_load(c, carry):
        pltpu.make_async_copy(mom_hbm.at[:, block(c, width)], mom.at[c], mom_sem).start()
        return carry

    def process(q, grad):
        momentum_out = beta_one * mom[q] + grad
        nesterov = grad + beta_one * momentum_out
        mom[q] = momentum_out
        panel = nesterov.astype(BF16)
        x[q] = panel
        norm[...] += nesterov * nesterov
        gram[...] += lax.dot_general(
            panel, panel, (((1,), (1,)), ((), ())), preferred_element_type=F32
        )

    def process_fin(p, c):
        arrived(fin.at[p, c], fin_sem.at[p, c])
        process(p * n + c, fin[p, c].astype(F32))

    @pl.when(is_end)
    def _():
        z_in = z + toward

        def og_to_inner(i):
            j = mirrored(nz - 1 - i)
            for k in range(ny):
                remote(
                    og_hbm.at[piece, rows_of(j)], ograw.at[ny + y, piece, rows_of(j)],
                    og_send.at[k], og_sem.at[ny + y, j, t], at(z_in, lax.rem(y + k, ny)),
                )

        def own_to_inner(c):
            remote(
                h_hbm.at[:, columns(y, c)], h.at[c, block(ny + y, tokens)],
                end_send, h_sem.at[ny + y, c], at(z_in, y),
            )

        og_to_inner(0)
        for c in range(min(2, n)):
            y_send(c)
        for i in range(1, nz):
            og_to_inner(i)
            if i <= min(end_ahead, n):
                own_to_inner(i - 1)
        for c in range(min(nz - 1, end_ahead, n), min(end_ahead, n)):
            own_to_inner(c)

        def rest(c, carry):
            y_send(c)
            return carry

        lax.fori_loop(min(2, n), n, rest, 0)
        lax.fori_loop(0, ny * n, mom_load, 0)
        gram[...] = jnp.zeros_like(gram)
        norm[...] = jnp.zeros_like(norm)

        def forward(c, carry):
            for k in range(1, ny):
                p = lax.rem(y + k, ny)
                arrived(h.at[c, block(p, tokens)], h_sem.at[p, c])
                remote(
                    h.at[c, block(p, tokens)], h.at[c, block(ny + p, tokens)],
                    fwd_send.at[k - 1], h_sem.at[ny + p, c], at(z_in, y),
                )

            @pl.when(c + end_ahead < n)
            def _():
                own_to_inner(c + end_ahead)

            return carry

        lax.fori_loop(0, n, forward, 0)
        pltpu.make_async_copy(mom, mom, mom_sem).wait()

        def finish(c, carry):
            for k in range(ny):
                process_fin(lax.rem(y + k, ny), c)
            return carry

        lax.fori_loop(0, n, finish, 0)

    @pl.when(jnp.logical_not(is_end))
    def _():
        near_end = inner_z == 1
        for i in range(nz):
            j = mirrored(nz - 1 - i)
            for k in range(1, ny):
                remote(
                    og_hbm.at[piece, rows_of(j)], ograw.at[y, piece, rows_of(j)],
                    og_send.at[k], og_sem.at[y, j, t], at_y(k),
                )
        for c in range(min(ahead, n)):
            y_send(c)
        pltpu.make_async_copy(og_hbm, ograw.at[y], og_own).start()

        def own_load(c, carry):
            pltpu.make_async_copy(
                h_hbm.at[:, columns(y, c)], h.at[c, block(y, tokens)], h_sem.at[y, c]
            ).start()
            return carry

        lax.fori_loop(0, n, own_load, 0)
        lax.fori_loop(0, ny * n, mom_load, 0)
        gram[...] = jnp.zeros_like(gram)
        norm[...] = jnp.zeros_like(norm)
        if half > 2:
            @pl.when(zm > 1)
            def _():
                h[:, ny * tokens :] = jnp.zeros((n, ny * tokens, width), BF16)
                ograw[ny:] = jnp.zeros((ny,) + ograw.shape[1:], BF16)

        pltpu.make_async_copy(mom, mom, mom_sem).wait()
        pltpu.make_async_copy(og_hbm, ograw.at[y], og_own).wait()

        def each_slot(fn):
            for k in range(1, ny):
                fn(lax.rem(y + k, ny))

            def from_end():
                for p in range(ny):
                    fn(ny + p)

            when(near_end, from_end)

        def og_piece(slot, tt, j):
            return ograw.at[slot, block(tt, tau), rows_of(j)]

        def to_core(slot, tt, j, k):
            remote(
                og_piece(slot, tt, j), og_piece(slot, tt, j),
                ogc_send.at[k], og_sem.at[slot, j, tt], at_t(tx * 2 + 1 - core),
            )

        def stage_a(i):
            j = mirrored(nz - 1 - i)

            def one(slot):
                arrived(og_piece(slot, t, j), og_sem.at[slot, j, t])
                for k in range(1, nx):
                    remote(
                        og_piece(slot, t, j), og_piece(slot, t, j),
                        ogx_send.at[k - 1], og_sem.at[slot, j, t],
                        at_t(lax.rem(tx + k, nx) * 2 + core),
                    )
                to_core(slot, t, j, 0)

            each_slot(one)

        def stage_b(i):
            j = mirrored(nz - 1 - i)

            def one(slot):
                for k in range(1, nx):
                    tt = lax.rem(tx + k, nx) * 2 + core
                    arrived(og_piece(slot, tt, j), og_sem.at[slot, j, tt])
                    to_core(slot, tt, j, k)

            each_slot(one)

        def stage_c(i):
            j = mirrored(nz - 1 - i)

            def one(slot):
                for k in range(nx):
                    tt = k * 2 + 1 - core
                    arrived(og_piece(slot, tt, j), og_sem.at[slot, j, tt])

            each_slot(one)
            for slot in range(slots if half == 2 else 0):
                for r in range(ny):
                    og_t[j, r * rows : (r + 1) * rows, slot * tokens : (slot + 1) * tokens] = (
                        ograw[slot, :, block(j * ny + r, rows)].T
                    )

        def partial(j, c):
            if half > 2:
                total = None
                for slot in range(slots):
                    term = lax.dot_general(
                        ograw[slot, :, rows_of(j)], h[c, slot * tokens : (slot + 1) * tokens],
                        (((0,), (0,)), ((), ())), preferred_element_type=F32,
                    )
                    total = term if total is None else total + term
                return total
            return jnp.dot(og_t[j], h[c], preferred_element_type=F32)

        def took(idx, c):
            arrived(recv.at[idx, c], recv_sem.at[idx, c])

        steps = n + (nz - 3) * lag + fin_lag

        def step(s, carry):
            f = s - (inner_z - 1) * lag
            f_on = jnp.logical_and(f >= 0, f < n)

            @pl.when(s == 0)
            def _():
                stage_a(0)

            def far(jm):
                j = mirrored(jm)

                def go():
                    own = partial(j, f)
                    if half == 2:
                        send[j, f] = own.astype(BF16)
                    else:
                        @pl.when(zm == 1)
                        def _():
                            send[j, f] = own.astype(BF16)

                        @pl.when(zm > 1)
                        def _():
                            took(far_slot(j), f)
                            send[j, f] = (own + recv[far_slot(j), f].astype(F32)).astype(BF16)

                    remote(
                        send.at[j, f], recv.at[far_slot(j), f],
                        s_send.at[j], recv_sem.at[far_slot(j), f], at(z + toward, y),
                    )

                if jm >= half:
                    pl.when(f_on)(go)
                else:
                    pl.when(jnp.logical_and(f_on, jm > zm))(go)

            for i in range(nz - 2):
                @pl.when(s == 0)
                def _():
                    stage_a(i + 1)
                    stage_b(i)
                    stage_c(i)

                if i == 0:
                    @pl.when(f_on)
                    def _():
                        arrived(h.at[f, block(y, tokens)], h_sem.at[y, f])
                        each_slot(lambda slot: arrived(h.at[f, block(slot, tokens)], h_sem.at[slot, f]))

                        @pl.when(f + ahead < n)
                        def _():
                            y_send(f + ahead)

                far(nz - 1 - i)

            @pl.when(s == 1)
            def _():
                stage_a(nz - 1)
                for i in range(nz - 2, nz):
                    stage_b(i)
                    stage_c(i)

            c = s - (nz - 2 - inner_z) * lag

            @pl.when(jnp.logical_and(c >= 0, c < n))
            def _():
                def near(jm):
                    j = mirrored(jm)
                    own = partial(j, c)
                    took(near_slot(j), c)
                    send[j, c] = (own + recv[near_slot(j), c].astype(F32)).astype(BF16)

                    def to_end():
                        for k in range(ny):
                            p = lax.rem(y + 1 + k, ny)
                            remote(
                                send.at[j, c, block(p, rows)], fin.at[y, c],
                                s_send.at[j], fin_sem.at[y, c], at(z_end, p),
                            )

                    def onward():
                        remote(
                            send.at[j, c], recv.at[near_slot(j), c],
                            s_send.at[j], recv_sem.at[near_slot(j), c], at(z - toward, y),
                        )

                    if jm > 0:
                        onward()
                    else:
                        when(near_end, to_end)
                        if half > 2:
                            pl.when(zm > 1)(onward)

                for jm in range(half - 1):
                    if jm == 0:
                        near(jm)
                    else:
                        pl.when(jm < zm)(functools.partial(near, jm))

                acc[...] = partial(z, c)
                took(near_slot(z), c)
                acc[...] += recv[near_slot(z), c].astype(F32)
                if half > 2:
                    @pl.when(zm > 1)
                    def _():
                        took(far_slot(z), c)
                        acc[...] += recv[far_slot(z), c].astype(F32)

                for k in range(1, ny):
                    p = lax.rem(y + k, ny)
                    send[z, c, block(p, rows)] = acc[block(p, rows)].astype(BF16)
                    remote(
                        send.at[z, c, block(p, rows)], fin.at[y, c],
                        s_send.at[z], fin_sem.at[y, c], at_y(k),
                    )
                process(y * n + c, acc[block(y, rows)])

            g = c - fin_lag

            @pl.when(jnp.logical_and(g >= 0, g < n))
            def _():
                for k in range(1, ny):
                    process_fin(lax.rem(y + k, ny), g)

            return carry

        lax.fori_loop(0, steps, step, 0)

    g_all[t, :rows] = gram[...]
    total = jnp.sum(jnp.sum(norm[...], axis=0, keepdims=True), axis=1, keepdims=True)
    g_all[t, rows:] = jnp.broadcast_to(total, (8, rows))
    for k in range(1, nt):
        pltpu.make_async_remote_copy(
            g_all.at[t], g_all.at[t], g_send.at[k - 1], g_recv.at[t],
            device_id=at_t(lax.rem(t + k, nt)), device_id_type=MESH,
        ).start()
    for k in range(nt):
        @pl.when(k != t)
        def _():
            pltpu.make_async_copy(g_all.at[k], g_all.at[k], g_recv.at[k]).wait()
    summed = g_all[0]
    for k in range(1, nt):
        summed = summed + g_all[k]
    inverse = 1.0 / (jnp.sqrt(summed[rows : rows + 1]) + 1e-07)
    current = summed[:rows] * inverse * inverse
    eye = (
        lax.broadcasted_iota(jnp.int32, (rows, rows), 0)
        == lax.broadcasted_iota(jnp.int32, (rows, rows), 1)
    ).astype(F32)
    map_all = None
    for iteration in range(ITERS):
        square = exact_dot(current, current)
        map_one = quintic_a * eye + quintic_b * current + quintic_c * square
        map_all = map_one if map_all is None else exact_dot(map_one, map_all)
        mapped = exact_dot(map_one, current)
        if iteration < ITERS - 1:
            current = exact_dot(mapped, map_one)
    energy = jnp.sum(mapped * map_one, axis=0, keepdims=True)
    second_out = beta_two * sec_ref[...] + (1.0 - beta_two) * energy
    secout_ref[...] = second_out
    scale = jnp.sqrt(ff / second_out) * inverse
    final = jnp.sum(eye * scale, axis=1, keepdims=True) * map_all
    final_ref[...] = final

    def sent(ref, sem):
        pltpu.make_async_copy(ref, ref, sem).wait()

    blocks = h.at[:, pl.ds(0, tokens)]
    og_piece_all = ograw.at[0, pl.ds(0, tau)]
    for k in range(1, ny):
        sent(blocks, hy_send.at[k - 1])
        sent(og_piece_all, og_send.at[k])

    @pl.when(is_end)
    def _():
        sent(og_piece_all, og_send.at[0])
        sent(blocks, end_send)
        for k in range(1, ny):
            sent(blocks, fwd_send.at[k - 1])

    @pl.when(jnp.logical_not(is_end))
    def _():
        def og_gather(count):
            pieces = ograw.at[pl.ds(0, count), pl.ds(0, tau)]
            for k in range(1, nx):
                sent(pieces, ogx_send.at[k - 1])
            for k in range(nx):
                sent(pieces, ogc_send.at[k])

        if half == 2:
            og_gather(slots - 1)
        else:
            pl.when(zm == 1)(functools.partial(og_gather, slots - 1))
            pl.when(zm > 1)(functools.partial(og_gather, ny - 1))
        for j in range(nz):
            @pl.when(z != j)
            def _():
                sent(send.at[j], s_send.at[j])

        if ny > 1:
            own = send.at[z, :, pl.ds(0, (ny - 1) * rows)]
            sent(own, s_send.at[z])

    for k in range(1, nt):
        sent(g_all.at[0], g_send.at[k - 1])


def write_kernel(n_chunks, x, mom, final_ref, sec_ref, upd_hbm, momout_hbm, secout_ref, out, mom_sem, upd_sem):
    width = x.shape[2]

    def columns(c):
        return pl.ds(pl.multiple_of(c * width, width), width)

    high = final_ref[...].astype(BF16)
    low = (final_ref[...] - high.astype(F32)).astype(BF16)
    secout_ref[...] = sec_ref[...]

    def finish(c, carry):
        pltpu.make_async_copy(mom.at[c], momout_hbm.at[:, columns(c)], mom_sem).start()
        panel = x[c]
        result = jnp.dot(high, panel, preferred_element_type=F32)
        result += jnp.dot(low, panel, preferred_element_type=F32)
        out[c] = result.astype(BF16)
        pltpu.make_async_copy(out.at[c], upd_hbm.at[:, columns(c)], upd_sem).start()
        return carry

    lax.fori_loop(0, n_chunks, finish, 0)
    pltpu.make_async_copy(mom, mom, mom_sem).wait()
    pltpu.make_async_copy(out, out, upd_sem).wait()


def body(nz, ny, nt, out_grad, hidden, momentum, second):
    tokens, cols = hidden.shape
    rows = momentum.shape[0]
    part = cols // ny
    width = 128
    n = part // width
    group = ny * rows
    dma = pltpu.SemaphoreType.DMA
    anywhere = pl.BlockSpec(memory_space=pltpu.HBM)
    vmem = pl.BlockSpec(memory_space=pltpu.VMEM)
    panel, mom, final, second_out = pl.pallas_call(
        functools.partial(kernel, nz, ny, nt, n, float(cols * nt)),
        out_shape=(
            jax.ShapeDtypeStruct((ny * n, rows, width), BF16),
            jax.ShapeDtypeStruct((ny * n, rows, width), F32),
            jax.ShapeDtypeStruct((rows, rows), F32),
            jax.ShapeDtypeStruct((1, rows), F32),
        ),
        in_specs=[anywhere, anywhere, anywhere, vmem],
        out_specs=(vmem, vmem, vmem, vmem),
        scratch_shapes=[
            pltpu.VMEM((n, 2 * ny * tokens, width), BF16),
            pltpu.VMEM((2 * ny, tokens, nz * group), BF16),
            pltpu.VMEM((nz if nz == 4 else 1, group, 2 * ny * tokens), BF16),
            pltpu.VMEM((nz + 1, n, group, width), BF16),
            pltpu.VMEM((nz, n, group, width), BF16),
            pltpu.VMEM((ny, n, rows, width), BF16),
            pltpu.VMEM((group, width), F32),
            pltpu.VMEM((rows, rows), F32),
            pltpu.VMEM((rows, width), F32),
            pltpu.VMEM((nt, rows + 8, rows), F32),
            dma((2 * ny, n)),
            dma((2 * ny, nz, nt)),
            dma,
            dma((nz + 1, n)),
            dma((ny, n)),
            dma,
            dma((max(ny - 1, 1),)),
            dma,
            dma((max(ny - 1, 1),)),
            dma((ny,)),
            dma((max(nt // 2 - 1, 1),)),
            dma((nt // 2,)),
            dma((nz,)),
            dma((max(nt - 1, 1),)),
            dma((nt,)),
        ],
        compiler_params=pltpu.CompilerParams(
            collective_id=0, has_side_effects=True, vmem_limit_bytes=59 * 1024 * 1024
        ),
        name="normuon",
    )(out_grad, hidden, momentum, second.reshape(1, rows))
    update, momentum_out, second_out = pl.pallas_call(
        functools.partial(write_kernel, ny * n),
        out_shape=(
            jax.ShapeDtypeStruct((rows, cols), BF16),
            jax.ShapeDtypeStruct((rows, cols), F32),
            jax.ShapeDtypeStruct((1, rows), F32),
        ),
        in_specs=[vmem] * 4,
        out_specs=(anywhere, anywhere, vmem),
        scratch_shapes=[pltpu.VMEM((ny * n, rows, width), BF16), dma, dma],
        compiler_params=pltpu.CompilerParams(vmem_limit_bytes=16 * 1024 * 1024),
        name="write_results",
    )(panel, mom, final, second_out)
    return update, momentum_out, second_out.reshape(rows)


def solution(mesh):
    nz, ny = line_split(mesh.shape["dp"])
    placed = (P("dp", None), P("dp", "tensor"), P("dp", "tensor"), P("dp"))
    return jax.shard_map(
        functools.partial(body, nz, ny, mesh.shape["tensor"]),
        mesh=mesh,
        in_specs=placed,
        out_specs=(P("dp", "tensor"), P("dp", "tensor"), P("dp")),
        check_vma=False,
    )
```

```python
import functools

import jax
import jax.numpy as jnp
from jax import lax
from jax.experimental import pallas as pl
from jax.experimental.pallas import tpu as pltpu
from jax.sharding import PartitionSpec as P

ITERS = 3
quintic_a = 3.4445
quintic_b = -4.775
quintic_c = 2.0315
beta_one = 0.95
beta_two = 0.95

MESH = pl.DeviceIdType.MESH
F32 = jnp.float32
BF16 = jnp.bfloat16


def line_split(n_dp):
    ny = 1
    while ny * ny * 4 <= n_dp and n_dp % (ny * 2) == 0:
        ny *= 2
    return n_dp // ny, ny


def exact_dot(a, b):
    return jnp.dot(a, b, preferred_element_type=F32, precision=lax.Precision.HIGHEST)


def kernel(
    nz, ny, nt, n, ff,
    og_hbm, h_hbm, mom_hbm, sec_hbm,
    x, mom, final_ref, secout_ref,
    h, ograw, og_t, recv, send, fin, acc, gram, g_all, sec_ref,
    h_sem, og_sem, og_own, recv_sem, fin_sem, mom_sem, sec_sem,
    hy_send, end_send, fwd_send, og_send, ogx_send, ogc_send, s_send, g_send, g_recv,
):
    tokens, part = h_hbm.shape[0], h_hbm.shape[1] // ny
    rows, width = x.shape[0], part // n
    group = ny * rows
    tau = tokens // nt
    nx = nt // 2
    slots = 2 * ny
    half = nz // 2
    ahead, end_ahead, lag, fin_lag = 6, 1, 2, 2
    d = lax.axis_index("dp")
    t = lax.axis_index("tensor")
    z, y = d // ny, lax.rem(d, ny)
    tx, core = t // 2, lax.rem(t, 2)
    lower = z * 2 < nz
    zm = jnp.where(lower, z, nz - 1 - z)
    toward = jnp.where(lower, 1, -1)
    is_end = zm == 0

    def mirrored(jm):
        return jnp.where(lower, jm, nz - 1 - jm)

    def far_slot(j):
        return jnp.where(lower, j + 1, j)

    def near_slot(j):
        return jnp.where(lower, j, j + 1)

    def at(zz, yy):
        return (zz * ny + yy, t)

    def at_y(k):
        return at(z, lax.rem(y + k, ny))

    def at_t(tt):
        return (d, tt)

    def when(cond, fn):
        if isinstance(cond, bool):
            if cond:
                fn()
        else:
            pl.when(cond)(fn)

    def remote(src, dst, send_sem, recv_sem, device):
        pltpu.make_async_remote_copy(
            src, dst, send_sem, recv_sem, device_id=device, device_id_type=MESH
        ).start()

    def arrived(ref, sem):
        pltpu.make_async_copy(ref, ref, sem).wait()

    def block(i, size):
        return pl.ds(pl.multiple_of(i * size, size), size)

    def columns(p, c):
        return block(p * n + c, width)

    inner_z = 1 if half == 2 else zm
    z_end = jnp.where(lower, 0, nz - 1)

    barrier = pltpu.get_barrier_semaphore()

    def hello(device):
        pl.semaphore_signal(barrier, inc=1, device_id=device, device_id_type=MESH)

    for k in range(1, ny):
        hello(at_y(k))
    for k in range(1, nt):
        hello(at_t(lax.rem(t + k, nt)))

    @pl.when(is_end)
    def _():
        for k in range(ny):
            hello(at(z + toward, k))

    @pl.when(jnp.logical_not(is_end))
    def _():
        hello(at(z + toward, y))

        def ends():
            for k in range(ny):
                hello(at(z_end, k))

        def next_in():
            hello(at(z - toward, y))

        if half == 2:
            ends()
        else:
            pl.when(zm == 1)(ends)
            pl.when(zm > 1)(next_in)

    greeted = (ny - 1) + (nt - 1)
    pl.semaphore_wait(
        barrier,
        greeted + jnp.where(zm == 0, ny, 0) + jnp.where(zm == 1, ny + 1, 0) + jnp.where(zm > 1, 2, 0),
    )

    def share(i, tt):
        if i == 0:
            return block(lax.rem(tt, 2), tokens // 2)
        return block(tt, tau)

    def rows_of(j):
        return block(j, group)

    def y_send(c):
        for k in range(1, ny):
            p = lax.rem(y + k, ny)
            remote(
                h_hbm.at[:, columns(p, c)], h.at[c, block(y, tokens)],
                hy_send.at[k - 1], h_sem.at[y, c], at_y(k),
            )

    def mom_load():
        pltpu.make_async_copy(mom_hbm, mom, mom_sem).start()
        pltpu.make_async_copy(sec_hbm, sec_ref, sec_sem).start()

    def process(q, grad):
        cols = block(q, width)
        momentum_out = beta_one * mom[:, cols] + grad
        mom[:, cols] = momentum_out
        panel = (grad + beta_one * momentum_out).astype(BF16)
        x[:, cols] = panel
        gram[...] += lax.dot_general(
            panel, panel, (((1,), (1,)), ((), ())), preferred_element_type=F32
        )

    def process_fin(p, c):
        arrived(fin.at[p, c], fin_sem.at[p, c])
        process(p * n + c, fin[p, c].astype(F32))

    @pl.when(is_end)
    def _():
        z_in = z + toward

        def og_to_inner(i):
            j = mirrored(nz - 1 - i)
            for k in range(ny):
                remote(
                    og_hbm.at[share(i, t), rows_of(j)], ograw.at[ny + y, share(i, t), rows_of(j)],
                    og_send.at[min(i, 1), k], og_sem.at[ny + y, j, t], at(z_in, lax.rem(y + k, ny)),
                )

        def own_to_inner(c):
            remote(
                h_hbm.at[:, columns(y, c)], h.at[c, block(ny + y, tokens)],
                end_send, h_sem.at[ny + y, c], at(z_in, y),
            )

        og_to_inner(0)
        for c in range(min(2, n)):
            y_send(c)
        for i in range(1, nz):
            og_to_inner(i)
            if i <= min(end_ahead, n):
                own_to_inner(i - 1)
        for c in range(min(nz - 1, end_ahead, n), min(end_ahead, n)):
            own_to_inner(c)

        def rest(c, carry):
            y_send(c)
            return carry

        lax.fori_loop(min(2, n), n, rest, 0)
        mom_load()
        gram[...] = jnp.zeros_like(gram)

        def forward(c, carry):
            for k in range(1, ny):
                p = lax.rem(y + k, ny)
                arrived(h.at[c, block(p, tokens)], h_sem.at[p, c])
                remote(
                    h.at[c, block(p, tokens)], h.at[c, block(ny + p, tokens)],
                    fwd_send.at[k - 1], h_sem.at[ny + p, c], at(z_in, y),
                )

            @pl.when(c + end_ahead < n)
            def _():
                own_to_inner(c + end_ahead)

            return carry

        lax.fori_loop(0, n, forward, 0)
        pltpu.make_async_copy(mom_hbm, mom, mom_sem).wait()
        pltpu.make_async_copy(sec_hbm, sec_ref, sec_sem).wait()

        def finish(c, carry):
            for k in range(ny):
                process_fin(lax.rem(y + k, ny), c)
            return carry

        lax.fori_loop(0, n, finish, 0)

    @pl.when(jnp.logical_not(is_end))
    def _():
        near_end = inner_z == 1
        for i in range(nz):
            j = mirrored(nz - 1 - i)
            for k in range(1, ny):
                remote(
                    og_hbm.at[share(i, t), rows_of(j)], ograw.at[y, share(i, t), rows_of(j)],
                    og_send.at[min(i, 1), k], og_sem.at[y, j, t], at_y(k),
                )
        for c in range(min(ahead, n)):
            y_send(c)
        pltpu.make_async_copy(og_hbm, ograw.at[y], og_own).start()

        def own_load(c, carry):
            pltpu.make_async_copy(
                h_hbm.at[:, columns(y, c)], h.at[c, block(y, tokens)], h_sem.at[y, c]
            ).start()
            return carry

        lax.fori_loop(0, n, own_load, 0)
        mom_load()
        gram[...] = jnp.zeros_like(gram)
        if half > 2:
            @pl.when(zm > 1)
            def _():
                h[:, ny * tokens :] = jnp.zeros((n, ny * tokens, width), BF16)
                ograw[ny:] = jnp.zeros((ny,) + ograw.shape[1:], BF16)

        pltpu.make_async_copy(mom_hbm, mom, mom_sem).wait()
        pltpu.make_async_copy(sec_hbm, sec_ref, sec_sem).wait()
        pltpu.make_async_copy(og_hbm, ograw.at[y], og_own).wait()

        def each_slot(fn):
            for k in range(1, ny):
                fn(lax.rem(y + k, ny))

            def from_end():
                for p in range(ny):
                    fn(ny + p)

            when(near_end, from_end)

        def og_piece(i, slot, tt):
            return ograw.at[slot, share(i, tt), rows_of(mirrored(nz - 1 - i))]

        def to_core(i, slot, tt, k):
            remote(
                og_piece(i, slot, tt), og_piece(i, slot, tt), ogc_send.at[min(i, 1), k],
                og_sem.at[slot, mirrored(nz - 1 - i), tt], at_t(tx * 2 + 1 - core),
            )

        def og_took(i, slot, tt):
            arrived(og_piece(i, slot, tt), og_sem.at[slot, mirrored(nz - 1 - i), tt])

        def stage_a(i):
            def one(slot):
                og_took(i, slot, t)
                if i > 0:
                    for k in range(1, nx):
                        remote(
                            og_piece(i, slot, t), og_piece(i, slot, t), ogx_send.at[k - 1],
                            og_sem.at[slot, mirrored(nz - 1 - i), t],
                            at_t(lax.rem(tx + k, nx) * 2 + core),
                        )
                to_core(i, slot, t, 0)

            each_slot(one)

        def stage_b(i):
            def one(slot):
                for k in range(1, nx):
                    tt = lax.rem(tx + k, nx) * 2 + core
                    og_took(i, slot, tt)
                    to_core(i, slot, tt, k)

            if i > 0:
                each_slot(one)

        def stage_c(i):
            j = mirrored(nz - 1 - i)

            def one(slot):
                if i == 0:
                    og_took(i, slot, tx * 2 + 1 - core)
                else:
                    for k in range(nx):
                        og_took(i, slot, k * 2 + 1 - core)

            each_slot(one)
            for slot in range(slots if half == 2 else 0):
                for r in range(ny):
                    og_t[j, r * rows : (r + 1) * rows, slot * tokens : (slot + 1) * tokens] = (
                        ograw[slot, :, block(j * ny + r, rows)].T
                    )

        def partial(j, c):
            if half > 2:
                total = None
                for slot in range(slots):
                    term = lax.dot_general(
                        ograw[slot, :, rows_of(j)], h[c, slot * tokens : (slot + 1) * tokens],
                        (((0,), (0,)), ((), ())), preferred_element_type=F32,
                    )
                    total = term if total is None else total + term
                return total
            return jnp.dot(og_t[j], h[c], preferred_element_type=F32)

        def took(idx, c):
            arrived(recv.at[idx, c], recv_sem.at[idx, c])

        steps = n + (nz - 3) * lag + fin_lag

        def step(s, carry):
            f = s - (inner_z - 1) * lag
            f_on = jnp.logical_and(f >= 0, f < n)

            @pl.when(s == 0)
            def _():
                stage_a(0)

            def far(jm):
                j = mirrored(jm)

                def go():
                    own = partial(j, f)
                    if half == 2:
                        send[j, f] = own.astype(BF16)
                    else:
                        @pl.when(zm == 1)
                        def _():
                            send[j, f] = own.astype(BF16)

                        @pl.when(zm > 1)
                        def _():
                            took(far_slot(j), f)
                            send[j, f] = (own + recv[far_slot(j), f].astype(F32)).astype(BF16)

                    remote(
                        send.at[j, f], recv.at[far_slot(j), f],
                        s_send.at[j], recv_sem.at[far_slot(j), f], at(z + toward, y),
                    )

                if jm >= half:
                    pl.when(f_on)(go)
                else:
                    pl.when(jnp.logical_and(f_on, jm > zm))(go)

            for i in range(nz - 2):
                @pl.when(s == 0)
                def _():
                    stage_a(i + 1)
                    stage_b(i)
                    stage_c(i)

                if i == 0:
                    @pl.when(f_on)
                    def _():
                        arrived(h.at[f, block(y, tokens)], h_sem.at[y, f])
                        each_slot(lambda slot: arrived(h.at[f, block(slot, tokens)], h_sem.at[slot, f]))

                        @pl.when(f + ahead < n)
                        def _():
                            y_send(f + ahead)

                far(nz - 1 - i)

            @pl.when(s == 1)
            def _():
                stage_a(nz - 1)
                for i in range(nz - 2, nz):
                    stage_b(i)
                    stage_c(i)

            c = s - (nz - 2 - inner_z) * lag

            @pl.when(jnp.logical_and(c >= 0, c < n))
            def _():
                def near(jm):
                    j = mirrored(jm)
                    own = partial(j, c)
                    took(near_slot(j), c)
                    send[j, c] = (own + recv[near_slot(j), c].astype(F32)).astype(BF16)

                    def to_end():
                        for k in range(ny):
                            p = lax.rem(y + 1 + k, ny)
                            remote(
                                send.at[j, c, block(p, rows)], fin.at[y, c],
                                s_send.at[j], fin_sem.at[y, c], at(z_end, p),
                            )

                    def onward():
                        remote(
                            send.at[j, c], recv.at[near_slot(j), c],
                            s_send.at[j], recv_sem.at[near_slot(j), c], at(z - toward, y),
                        )

                    if jm > 0:
                        onward()
                    else:
                        when(near_end, to_end)
                        if half > 2:
                            pl.when(zm > 1)(onward)

                for jm in range(half - 1):
                    if jm == 0:
                        near(jm)
                    else:
                        pl.when(jm < zm)(functools.partial(near, jm))

                acc[...] = partial(z, c)
                took(near_slot(z), c)
                acc[...] += recv[near_slot(z), c].astype(F32)
                if half > 2:
                    @pl.when(zm > 1)
                    def _():
                        took(far_slot(z), c)
                        acc[...] += recv[far_slot(z), c].astype(F32)

                for k in range(1, ny):
                    p = lax.rem(y + k, ny)
                    send[z, c, block(p, rows)] = acc[block(p, rows)].astype(BF16)
                    remote(
                        send.at[z, c, block(p, rows)], fin.at[y, c],
                        s_send.at[z], fin_sem.at[y, c], at_y(k),
                    )
                process(y * n + c, acc[block(y, rows)])

            g = c - fin_lag

            @pl.when(jnp.logical_and(g >= 0, g < n))
            def _():
                for k in range(1, ny):
                    process_fin(lax.rem(y + k, ny), g)

            return carry

        lax.fori_loop(0, steps, step, 0)

    g_all[t] = gram[...].astype(BF16)
    for k in range(1, nt):
        pltpu.make_async_remote_copy(
            g_all.at[t], g_all.at[t], g_send.at[k - 1], g_recv.at[t],
            device_id=at_t(lax.rem(t + k, nt)), device_id_type=MESH,
        ).start()
    for k in range(nt):
        @pl.when(k != t)
        def _():
            pltpu.make_async_copy(g_all.at[k], g_all.at[k], g_recv.at[k]).wait()
    summed = g_all[0].astype(F32)
    for k in range(1, nt):
        summed = summed + g_all[k].astype(F32)
    eye = (
        lax.broadcasted_iota(jnp.int32, (rows, rows), 0)
        == lax.broadcasted_iota(jnp.int32, (rows, rows), 1)
    ).astype(F32)
    total = jnp.sum(jnp.sum(summed * eye, axis=0, keepdims=True), axis=1, keepdims=True)
    inverse = 1.0 / (jnp.sqrt(total) + 1e-07)
    current = summed * inverse * inverse
    map_all = None
    for iteration in range(ITERS):
        square = exact_dot(current, current)
        map_one = quintic_a * eye + quintic_b * current + quintic_c * square
        map_all = map_one if map_all is None else exact_dot(map_one, map_all)
        mapped = exact_dot(map_one, current)
        if iteration < ITERS - 1:
            current = exact_dot(mapped, map_one)
    energy = jnp.sum(mapped * map_one, axis=0, keepdims=True)
    second_out = beta_two * sec_ref[...] + (1.0 - beta_two) * energy
    secout_ref[...] = second_out
    scale = jnp.sqrt(ff / second_out) * inverse
    final = jnp.sum(eye * scale, axis=1, keepdims=True) * map_all
    final_ref[...] = final

    def sent(ref, sem):
        pltpu.make_async_copy(ref, ref, sem).wait()

    blocks = h.at[:, pl.ds(0, tokens)]

    def og_sent(k):
        sent(ograw.at[0, pl.ds(0, tokens // 2), pl.ds(0, group)], og_send.at[0, k])
        sent(ograw.at[0, pl.ds(0, tau), pl.ds(0, (nz - 1) * group)], og_send.at[1, k])

    for k in range(1, ny):
        sent(blocks, hy_send.at[k - 1])
        og_sent(k)

    @pl.when(is_end)
    def _():
        og_sent(0)
        sent(blocks, end_send)
        for k in range(1, ny):
            sent(blocks, fwd_send.at[k - 1])

    @pl.when(jnp.logical_not(is_end))
    def _():
        def og_gather(count):
            pieces = ograw.at[pl.ds(0, count), pl.ds(0, tau), pl.ds(0, (nz - 1) * group)]
            sent(ograw.at[pl.ds(0, count), pl.ds(0, tokens // 2), pl.ds(0, group)], ogc_send.at[0, 0])
            for k in range(1, nx):
                sent(pieces, ogx_send.at[k - 1])
            for k in range(nx):
                sent(pieces, ogc_send.at[1, k])

        if half == 2:
            og_gather(slots - 1)
        else:
            pl.when(zm == 1)(functools.partial(og_gather, slots - 1))
            pl.when(zm > 1)(functools.partial(og_gather, ny - 1))
        for j in range(nz):
            @pl.when(z != j)
            def _():
                sent(send.at[j], s_send.at[j])

        if ny > 1:
            own = send.at[z, :, pl.ds(0, (ny - 1) * rows)]
            sent(own, s_send.at[z])

    for k in range(1, nt):
        sent(g_all.at[0], g_send.at[k - 1])


def write_kernel(x, mom, final_ref, sec_ref, upd_hbm, momout_hbm, secout_ref, out, mom_sem, upd_sem):
    pltpu.make_async_copy(mom, momout_hbm, mom_sem).start()
    high = final_ref[...].astype(BF16)
    secout_ref[...] = sec_ref[...]
    cols = x.shape[1]
    width = 512 if cols % 512 == 0 else 128
    n = cols // width

    def finish(c, carry):
        part = pl.ds(pl.multiple_of(c * width, width), width)
        out[:, part] = jnp.dot(high, x[:, part], preferred_element_type=F32).astype(BF16)
        pltpu.make_async_copy(out.at[:, part], upd_hbm.at[:, part], upd_sem.at[0]).start()
        return carry

    lax.fori_loop(0, n, finish, 0)
    pltpu.make_async_copy(mom, momout_hbm, mom_sem).wait()
    pltpu.make_async_copy(out, upd_hbm, upd_sem.at[0]).wait()


def body(nz, ny, nt, out_grad, hidden, momentum, second):
    tokens, cols = hidden.shape
    rows = momentum.shape[0]
    part = cols // ny
    width = 128
    n = part // width
    group = ny * rows
    dma = pltpu.SemaphoreType.DMA
    anywhere = pl.BlockSpec(memory_space=pltpu.HBM)
    vmem = pl.BlockSpec(memory_space=pltpu.VMEM)
    panel, mom, final, second_out = pl.pallas_call(
        functools.partial(kernel, nz, ny, nt, n, float(cols * nt)),
        out_shape=(
            jax.ShapeDtypeStruct((rows, cols), BF16),
            jax.ShapeDtypeStruct((rows, cols), F32),
            jax.ShapeDtypeStruct((rows, rows), F32),
            jax.ShapeDtypeStruct((1, rows), F32),
        ),
        in_specs=[anywhere] * 4,
        out_specs=(vmem, vmem, vmem, vmem),
        scratch_shapes=[
            pltpu.VMEM((n, 2 * ny * tokens, width), BF16),
            pltpu.VMEM((2 * ny, tokens, nz * group), BF16),
            pltpu.VMEM((nz if nz == 4 else 1, group, 2 * ny * tokens), BF16),
            pltpu.VMEM((nz + 1, n, group, width), BF16),
            pltpu.VMEM((nz, n, group, width), BF16),
            pltpu.VMEM((ny, n, rows, width), BF16),
            pltpu.VMEM((group, width), F32),
            pltpu.VMEM((rows, rows), F32),
            pltpu.VMEM((nt, rows, rows), BF16),
            pltpu.VMEM((1, rows), F32),
            dma((2 * ny, n)),
            dma((2 * ny, nz, nt)),
            dma,
            dma((nz + 1, n)),
            dma((ny, n)),
            dma,
            dma,
            dma((max(ny - 1, 1),)),
            dma,
            dma((max(ny - 1, 1),)),
            dma((2, ny)),
            dma((max(nt // 2 - 1, 1),)),
            dma((2, nt // 2)),
            dma((nz,)),
            dma((max(nt - 1, 1),)),
            dma((nt,)),
        ],
        compiler_params=pltpu.CompilerParams(
            collective_id=0, has_side_effects=True, vmem_limit_bytes=48 * 1024 * 1024
        ),
        name="normuon",
    )(
        *(
            pltpu.with_memory_space_constraint(v, pltpu.HBM)
            for v in (out_grad, hidden, momentum, second.reshape(1, rows))
        )
    )
    update, momentum_out, second_out = pl.pallas_call(
        write_kernel,
        out_shape=(
            jax.ShapeDtypeStruct((rows, cols), BF16),
            jax.ShapeDtypeStruct((rows, cols), F32),
            jax.ShapeDtypeStruct((1, rows), F32),
        ),
        in_specs=[vmem] * 4,
        out_specs=(anywhere, anywhere, vmem),
        scratch_shapes=[pltpu.VMEM((rows, cols), BF16), dma, dma((2,))],
        compiler_params=pltpu.CompilerParams(vmem_limit_bytes=16 * 1024 * 1024),
        name="write_results",
    )(panel, mom, final, second_out)
    return update, momentum_out, second_out.reshape(rows)


def solution(mesh):
    nz, ny = line_split(mesh.shape["dp"])
    placed = (P("dp", None), P("dp", "tensor"), P("dp", "tensor"), P("dp"))
    return jax.shard_map(
        functools.partial(body, nz, ny, mesh.shape["tensor"]),
        mesh=mesh,
        in_specs=placed,
        out_specs=(P("dp", "tensor"), P("dp", "tensor"), P("dp")),
        check_vma=False,
    )
```

```python
import functools

import jax
import jax.numpy as jnp
from jax import lax
from jax.experimental import pallas as pl
from jax.experimental.pallas import tpu as pltpu
from jax.sharding import PartitionSpec as P

ITERS = 3
quintic_a = 3.4445
quintic_b = -4.775
quintic_c = 2.0315
beta_one = 0.95
beta_two = 0.95

MESH = pl.DeviceIdType.MESH
F32 = jnp.float32
BF16 = jnp.bfloat16


def line_split(n_dp):
    ny = 1
    while ny * ny * 4 <= n_dp and n_dp % (ny * 2) == 0:
        ny *= 2
    return n_dp // ny, ny


def exact_dot(a, b):
    return jnp.dot(a, b, preferred_element_type=F32, precision=lax.Precision.HIGHEST)


def kernel(
    nz, ny, nt, n, ff,
    og_hbm, h_hbm, mom_hbm, sec_hbm,
    x, mom, final_ref, secout_ref,
    h, ograw, og_t, recv, send, fin, acc, gram, g_all, sec_ref,
    h_sem, og_sem, og_own, ogy_send, recv_sem, fin_sem, mom_sem, sec_sem,
    hy_send, end_send, fwd_send, og_send, ogx_send, ogc_send, s_send, g_send, g_recv,
):
    tokens, part = h_hbm.shape[0], h_hbm.shape[1] // ny
    rows, width = x.shape[0], part // n
    group = ny * rows
    tau = tokens // nt
    nx = nt // 2
    slots = 2 * ny
    half = nz // 2
    ahead, end_ahead, lag, late, fin_lag = nz + 1, 1, 2, 6, 2
    d = lax.axis_index("dp")
    t = lax.axis_index("tensor")
    z, y = d // ny, lax.rem(d, ny)
    tx, core = t // 2, lax.rem(t, 2)
    lower = z * 2 < nz
    zm = jnp.where(lower, z, nz - 1 - z)
    toward = jnp.where(lower, 1, -1)
    is_end = zm == 0

    def mirrored(jm):
        return jnp.where(lower, jm, nz - 1 - jm)

    def far_slot(jm):
        return half + jm

    def onward_slot(jm):
        if half == 2:
            return nz - 1 - jm
        return jnp.where(zm == half - 1, nz - 1 - jm, far_slot(jm))

    def at(zz, yy):
        return (zz * ny + yy, t)

    def at_y(k):
        return at(z, lax.rem(y + k, ny))

    def at_t(tt):
        return (d, tt)

    def when(cond, fn):
        if isinstance(cond, bool):
            if cond:
                fn()
        else:
            pl.when(cond)(fn)

    def remote(src, dst, send_sem, recv_sem, device):
        pltpu.make_async_remote_copy(
            src, dst, send_sem, recv_sem, device_id=device, device_id_type=MESH
        ).start()

    def arrived(ref, sem):
        pltpu.make_async_copy(ref, ref, sem).wait()

    def block(i, size):
        return pl.ds(pl.multiple_of(i * size, size), size)

    def columns(p, c):
        return block(p * n + c, width)

    inner_z = 1 if half == 2 else zm
    z_end = jnp.where(lower, 0, nz - 1)

    barrier = pltpu.get_barrier_semaphore()

    def hello(device):
        pl.semaphore_signal(barrier, inc=1, device_id=device, device_id_type=MESH)

    for k in range(1, ny):
        hello(at_y(k))
    for k in range(1, nt):
        hello(at_t(lax.rem(t + k, nt)))

    @pl.when(is_end)
    def _():
        for k in range(ny):
            hello(at(z + toward, k))

    @pl.when(jnp.logical_not(is_end))
    def _():
        hello(at(z + toward, y))

        def ends():
            for k in range(ny):
                hello(at(z_end, k))

        def next_in():
            hello(at(z - toward, y))

        if half == 2:
            ends()
        else:
            pl.when(zm == 1)(ends)
            pl.when(zm > 1)(next_in)

    greeted = (ny - 1) + (nt - 1)
    pl.semaphore_wait(
        barrier,
        greeted + jnp.where(zm == 0, ny, 0) + jnp.where(zm == 1, ny + 1, 0) + jnp.where(zm > 1, 2, 0),
    )

    def share(i, tt):
        if i == 0:
            return block(lax.rem(tt, 2), tokens // 2)
        return block(tt, tau)

    def rows_of(j):
        return block(j, group)

    def y_send(c):
        for k in range(1, ny):
            p = lax.rem(y + k, ny)
            remote(
                h_hbm.at[:, columns(p, c)], h.at[c, block(y, tokens)],
                hy_send.at[k - 1], h_sem.at[c], at_y(k),
            )

    def mom_load():
        pltpu.make_async_copy(mom_hbm, mom, mom_sem).start()
        pltpu.make_async_copy(sec_hbm, sec_ref, sec_sem).start()

    def process(q, grad):
        cols = block(q, width)
        momentum_out = beta_one * mom[:, cols] + grad
        mom[:, cols] = momentum_out
        panel = (grad + beta_one * momentum_out).astype(BF16)
        x[:, cols] = panel
        gram[...] += lax.dot_general(
            panel, panel, (((1,), (1,)), ((), ())), preferred_element_type=F32
        )

    def process_fin(count, c):
        arrived(fin.at[c, pl.ds(0, count)], fin_sem.at[c])
        for k in range(ny - count, ny):
            p = lax.rem(y + k, ny)
            process(p * n + c, fin[c, p].astype(F32))

    @pl.when(is_end)
    def _():
        z_in = z + toward

        def og_to_inner(i):
            j = mirrored(nz - 1 - i)
            remote(
                og_hbm.at[share(i, t), rows_of(j)], ograw.at[ny + y, share(i, t), rows_of(j)],
                og_send.at[min(i, 1), 0], og_sem.at[ny + y, j, t], at(z_in, y),
            )

        def own_to_inner(c):
            remote(
                h_hbm.at[:, columns(y, c)], h.at[c, block(ny + y, tokens)],
                end_send, h_sem.at[c], at(z_in, y),
            )

        og_to_inner(0)
        for c in range(min(2, n)):
            y_send(c)
        for i in range(1, nz - 2):
            og_to_inner(i)
        for c in range(min(end_ahead, n)):
            own_to_inner(c)

        def rest(c, carry):
            y_send(c)
            return carry

        lax.fori_loop(min(2, n), n, rest, 0)
        mom_load()
        gram[...] = jnp.zeros_like(gram)

        def forward(c, carry):
            arrived(h.at[c, pl.ds(0, (ny - 1) * tokens)], h_sem.at[c])
            for k in range(1, ny):
                p = lax.rem(y + k, ny)
                remote(
                    h.at[c, block(p, tokens)], h.at[c, block(ny + p, tokens)],
                    fwd_send.at[k - 1], h_sem.at[c], at(z_in, y),
                )

            @pl.when(c + end_ahead < n)
            def _():
                own_to_inner(c + end_ahead)

            @pl.when(c == min(2, n) - 1)
            def _():
                for i in range(nz - 2, nz):
                    og_to_inner(i)

            return carry

        lax.fori_loop(0, n, forward, 0)
        pltpu.make_async_copy(mom_hbm, mom, mom_sem).wait()
        pltpu.make_async_copy(sec_hbm, sec_ref, sec_sem).wait()

        def finish(c, carry):
            process_fin(ny, c)
            return carry

        lax.fori_loop(0, n, finish, 0)

    @pl.when(jnp.logical_not(is_end))
    def _():
        near_end = inner_z == 1
        def og_to_peers(i):
            j = mirrored(nz - 1 - i)
            for k in range(1, ny):
                remote(
                    og_hbm.at[share(i, t), rows_of(j)], ograw.at[y, share(i, t), rows_of(j)],
                    og_send.at[min(i, 1), k], og_sem.at[y, j, t], at_y(k),
                )

        og_to_peers(0)
        y_send(0)
        for i in range(1, nz - 2):
            og_to_peers(i)
        pltpu.make_async_copy(og_hbm, ograw.at[y], og_own).start()

        def own_load(c, carry):
            pltpu.make_async_copy(
                h_hbm.at[:, columns(y, c)], h.at[c, block(y, tokens)], h_sem.at[c]
            ).start()
            return carry

        lax.fori_loop(0, n, own_load, 0)
        mom_load()
        gram[...] = jnp.zeros_like(gram)
        if half > 2:
            @pl.when(zm > 1)
            def _():
                h[:, ny * tokens :] = jnp.zeros((n, ny * tokens, width), BF16)
                ograw[ny:] = jnp.zeros((ny,) + ograw.shape[1:], BF16)

        pltpu.make_async_copy(og_hbm, ograw.at[y], og_own).wait()

        def peer_slots(fn):
            for k in range(1, ny):
                fn(lax.rem(y + k, ny))

            def from_end():
                for k in range(1, ny):
                    fn(ny + lax.rem(y + k, ny))

            when(near_end, from_end)

        def each_slot(fn):
            peer_slots(fn)
            when(near_end, functools.partial(fn, ny + y))

        def og_piece(i, slot, tt):
            return ograw.at[slot, share(i, tt), rows_of(mirrored(nz - 1 - i))]

        def to_core(i, slot, tt, k):
            remote(
                og_piece(i, slot, tt), og_piece(i, slot, tt), ogc_send.at[min(i, 1), k],
                og_sem.at[slot, mirrored(nz - 1 - i), tt], at_t(tx * 2 + 1 - core),
            )

        def og_took(i, slot, tt):
            arrived(og_piece(i, slot, tt), og_sem.at[slot, mirrored(nz - 1 - i), tt])

        def share_out(i, slot):
            if i > 0:
                for k in range(1, nx):
                    remote(
                        og_piece(i, slot, t), og_piece(i, slot, t), ogx_send.at[k - 1],
                        og_sem.at[slot, mirrored(nz - 1 - i), t],
                        at_t(lax.rem(tx + k, nx) * 2 + core),
                    )
            to_core(i, slot, t, 0)

        def stage_end(i):
            def go():
                og_took(i, ny + y, t)
                for k in range(1, ny):
                    remote(
                        og_piece(i, ny + y, t), og_piece(i, ny + y, t), ogy_send.at[min(i, 1), k - 1],
                        og_sem.at[ny + y, mirrored(nz - 1 - i), t], at_y(k),
                    )
                share_out(i, ny + y)

            when(near_end, go)

        def stage_a(i):
            def one(slot):
                og_took(i, slot, t)
                share_out(i, slot)

            peer_slots(one)

        def stage_b(i):
            def one(slot):
                for k in range(1, nx):
                    tt = lax.rem(tx + k, nx) * 2 + core
                    og_took(i, slot, tt)
                    to_core(i, slot, tt, k)

            if i > 0:
                each_slot(one)

        def stage_c(i):
            j = mirrored(nz - 1 - i)

            def one(slot):
                if i == 0:
                    og_took(i, slot, tx * 2 + 1 - core)
                else:
                    for k in range(nx):
                        og_took(i, slot, k * 2 + 1 - core)

            each_slot(one)
            for slot in range(slots if half == 2 else 0):
                for r in range(ny):
                    og_t[j, r * rows : (r + 1) * rows, slot * tokens : (slot + 1) * tokens] = (
                        ograw[slot, :, block(j * ny + r, rows)].T
                    )

        def partial(j, c):
            if half > 2:
                total = None
                for slot in range(slots):
                    term = lax.dot_general(
                        ograw[slot, :, rows_of(j)], h[c, slot * tokens : (slot + 1) * tokens],
                        (((0,), (0,)), ((), ())), preferred_element_type=F32,
                    )
                    total = term if total is None else total + term
                return total
            return jnp.dot(og_t[j], h[c], preferred_element_type=F32)

        def took(idx, c):
            arrived(recv.at[idx, c], recv_sem.at[idx, c])

        steps = n + max((nz - 3) * lag, late) + fin_lag

        def step(s, carry):
            first = s - (inner_z - 1) * lag

            @pl.when(s == 0)
            def _():
                for i in range(nz - 2):
                    stage_end(i)
                if 1 < min(ahead, n):
                    y_send(1)
                for i in range(nz - 2, nz):
                    og_to_peers(i)
                for c in range(2, min(ahead, n)):
                    y_send(c)
                for i in range(nz - 2):
                    stage_a(i)
                stage_c(0)

            @pl.when(jnp.logical_and(first >= 0, first < n))
            def _():
                def took_hidden(count):
                    arrived(h.at[first, pl.ds(0, count * tokens)], h_sem.at[first])

                if half == 2:
                    took_hidden(slots)
                else:
                    pl.when(zm == 1)(functools.partial(took_hidden, slots))
                    pl.when(zm > 1)(functools.partial(took_hidden, ny))

                @pl.when(first + ahead < n)
                def _():
                    y_send(first + ahead)

            def far(jm, f):
                j = mirrored(jm)
                own = partial(j, f)
                if half == 2:
                    send[j, f] = own.astype(BF16)
                else:
                    @pl.when(zm == 1)
                    def _():
                        send[j, f] = own.astype(BF16)

                    @pl.when(zm > 1)
                    def _():
                        took(far_slot(jm), f)
                        send[j, f] = (own + recv[far_slot(jm), f].astype(F32)).astype(BF16)

                remote(
                    send.at[j, f], recv.at[onward_slot(jm), f],
                    s_send.at[j], recv_sem.at[onward_slot(jm), f], at(z + toward, y),
                )

            @pl.when(jnp.logical_and(first >= 0, first < n))
            def _():
                far(nz - 1, first)


            @pl.when(s == 1)
            def _():
                for i in range(1, nz - 2):
                    stage_b(i)
                    stage_c(i)

            def done_later(v):
                return jnp.clip(jnp.where(v < 2, v, v + 1), 0, n)

            def later(f, carry):
                for jm in range(nz - 2, 1, -1):
                    if jm >= half:
                        far(jm, f)
                    else:
                        pl.when(jm > zm)(functools.partial(far, jm, f))
                return carry

            lax.fori_loop(done_later(first - 1), done_later(first), later, 0)

            @pl.when(s == 2)
            def _():
                for i in range(nz - 2, nz):
                    stage_end(i)

            @pl.when(s == 3)
            def _():
                for i in range(nz - 2, nz):
                    stage_a(i)

            @pl.when(s == 4)
            def _():
                for i in range(nz - 2, nz):
                    stage_b(i)

            @pl.when(s == late - 1)
            def _():
                for i in range(nz - 2, nz):
                    stage_c(i)
                pltpu.make_async_copy(mom_hbm, mom, mom_sem).wait()
                pltpu.make_async_copy(sec_hbm, sec_ref, sec_sem).wait()

            near_lag = (nz - 2 - inner_z) * lag

            def done_near(v):
                return jnp.clip(jnp.minimum(2 * (v + 1 - late), v + 1 - near_lag), 0, n)

            def near_chunk(c, carry):
                def near(jm):
                    j = mirrored(jm)
                    own = partial(j, c)
                    took(jm, c)
                    send[j, c] = (own + recv[jm, c].astype(F32)).astype(BF16)

                    def to_end():
                        for k in range(ny):
                            p = lax.rem(y + 1 + k, ny)
                            remote(
                                send.at[j, c, block(p, rows)], fin.at[c, y],
                                s_send.at[j], fin_sem.at[c], at(z_end, p),
                            )

                    def onward():
                        remote(
                            send.at[j, c], recv.at[jm, c],
                            s_send.at[j], recv_sem.at[jm, c], at(z - toward, y),
                        )

                    if jm > 0:
                        onward()
                    else:
                        when(near_end, to_end)
                        if half > 2:
                            pl.when(zm > 1)(onward)

                for jm in range(half - 1):
                    if jm == 0:
                        near(jm)
                    else:
                        pl.when(jm < zm)(functools.partial(near, jm))

                acc[...] = partial(z, c)
                took(inner_z, c)
                acc[...] += recv[inner_z, c].astype(F32)
                if half > 2:
                    @pl.when(zm > 1)
                    def _():
                        took(far_slot(zm), c)
                        acc[...] += recv[far_slot(zm), c].astype(F32)

                for k in range(1, ny):
                    p = lax.rem(y + k, ny)
                    send[z, c, block(p, rows)] = acc[block(p, rows)].astype(BF16)
                    remote(
                        send.at[z, c, block(p, rows)], fin.at[c, y],
                        s_send.at[z], fin_sem.at[c], at_y(k),
                    )
                process(y * n + c, acc[block(y, rows)])
                return carry

            def fin_chunk(c, carry):
                process_fin(ny - 1, c)
                return carry

            lax.fori_loop(done_near(s - 1), done_near(s), near_chunk, 0)
            lax.fori_loop(done_near(s - 1 - fin_lag), done_near(s - fin_lag), fin_chunk, 0)
            return carry

        lax.fori_loop(0, steps, step, 0)

    g_all[t] = gram[...].astype(BF16)
    for k in range(1, nt):
        pltpu.make_async_remote_copy(
            g_all.at[t], g_all.at[t], g_send.at[k - 1], g_recv.at[t],
            device_id=at_t(lax.rem(t + k, nt)), device_id_type=MESH,
        ).start()
    for k in range(nt):
        @pl.when(k != t)
        def _():
            pltpu.make_async_copy(g_all.at[k], g_all.at[k], g_recv.at[k]).wait()
    summed = g_all[0].astype(F32)
    for k in range(1, nt):
        summed = summed + g_all[k].astype(F32)
    eye = (
        lax.broadcasted_iota(jnp.int32, (rows, rows), 0)
        == lax.broadcasted_iota(jnp.int32, (rows, rows), 1)
    ).astype(F32)
    total = jnp.sum(jnp.sum(summed * eye, axis=0, keepdims=True), axis=1, keepdims=True)
    inverse = 1.0 / (jnp.sqrt(total) + 1e-07)
    current = summed * inverse * inverse
    map_all = None
    for iteration in range(ITERS):
        square = exact_dot(current, current)
        map_one = quintic_a * eye + quintic_b * current + quintic_c * square
        map_all = map_one if map_all is None else exact_dot(map_one, map_all)
        mapped = exact_dot(map_one, current)
        if iteration < ITERS - 1:
            current = exact_dot(mapped, map_one)
    energy = jnp.sum(mapped * map_one, axis=0, keepdims=True)
    second_out = beta_two * sec_ref[...] + (1.0 - beta_two) * energy
    secout_ref[...] = second_out
    scale = jnp.sqrt(ff / second_out) * inverse
    final = jnp.sum(eye * scale, axis=1, keepdims=True) * map_all
    final_ref[...] = final

    def sent(ref, sem):
        pltpu.make_async_copy(ref, ref, sem).wait()

    blocks = h.at[:, pl.ds(0, tokens)]

    def og_sent(sems, k):
        sent(ograw.at[0, pl.ds(0, tokens // 2), pl.ds(0, group)], sems.at[0, k])
        sent(ograw.at[0, pl.ds(0, tau), pl.ds(0, (nz - 1) * group)], sems.at[1, k])

    for k in range(1, ny):
        sent(blocks, hy_send.at[k - 1])

    @pl.when(is_end)
    def _():
        og_sent(og_send, 0)
        sent(blocks, end_send)
        for k in range(1, ny):
            sent(blocks, fwd_send.at[k - 1])

    @pl.when(jnp.logical_not(is_end))
    def _():
        def og_forwarded():
            for k in range(1, ny):
                og_sent(ogy_send, k - 1)

        for k in range(1, ny):
            og_sent(og_send, k)
        if half == 2:
            og_forwarded()
        else:
            pl.when(zm == 1)(og_forwarded)

        def og_gather(count):
            pieces = ograw.at[pl.ds(0, count), pl.ds(0, tau), pl.ds(0, (nz - 1) * group)]
            sent(ograw.at[pl.ds(0, count), pl.ds(0, tokens // 2), pl.ds(0, group)], ogc_send.at[0, 0])
            for k in range(1, nx):
                sent(pieces, ogx_send.at[k - 1])
            for k in range(nx):
                sent(pieces, ogc_send.at[1, k])

        if half == 2:
            og_gather(slots - 1)
        else:
            pl.when(zm == 1)(functools.partial(og_gather, slots - 1))
            pl.when(zm > 1)(functools.partial(og_gather, ny - 1))
        for j in range(nz):
            @pl.when(z != j)
            def _():
                sent(send.at[j], s_send.at[j])

        if ny > 1:
            own = send.at[z, :, pl.ds(0, (ny - 1) * rows)]
            sent(own, s_send.at[z])

    for k in range(1, nt):
        sent(g_all.at[0], g_send.at[k - 1])


def write_kernel(x, mom, final_ref, sec_ref, upd_hbm, momout_hbm, secout_ref, out, mom_sem, upd_sem):
    pltpu.make_async_copy(mom, momout_hbm, mom_sem).start()
    high = final_ref[...].astype(BF16)
    secout_ref[...] = sec_ref[...]
    cols = x.shape[1]
    width = 512 if cols % 512 == 0 else 128
    n = cols // width

    def finish(c, carry):
        part = pl.ds(pl.multiple_of(c * width, width), width)
        out[:, part] = jnp.dot(high, x[:, part], preferred_element_type=F32).astype(BF16)
        pltpu.make_async_copy(out.at[:, part], upd_hbm.at[:, part], upd_sem.at[0]).start()
        return carry

    lax.fori_loop(0, n, finish, 0)
    pltpu.make_async_copy(mom, momout_hbm, mom_sem).wait()
    pltpu.make_async_copy(out, upd_hbm, upd_sem.at[0]).wait()


def body(nz, ny, nt, out_grad, hidden, momentum, second):
    tokens, cols = hidden.shape
    rows = momentum.shape[0]
    part = cols // ny
    width = 128
    n = part // width
    group = ny * rows
    recv_slots = nz // 2 if nz == 4 else nz // 2 + nz
    dma = pltpu.SemaphoreType.DMA
    anywhere = pl.BlockSpec(memory_space=pltpu.HBM)
    vmem = pl.BlockSpec(memory_space=pltpu.VMEM)
    panel, mom, final, second_out = pl.pallas_call(
        functools.partial(kernel, nz, ny, nt, n, float(cols * nt)),
        out_shape=(
            jax.ShapeDtypeStruct((rows, cols), BF16),
            jax.ShapeDtypeStruct((rows, cols), F32),
            jax.ShapeDtypeStruct((rows, rows), F32),
            jax.ShapeDtypeStruct((1, rows), F32),
        ),
        in_specs=[anywhere] * 4,
        out_specs=(vmem, vmem, vmem, vmem),
        scratch_shapes=[
            pltpu.VMEM((n, 2 * ny * tokens, width), BF16),
            pltpu.VMEM((2 * ny, tokens, nz * group), BF16),
            pltpu.VMEM((nz if nz == 4 else 1, group, 2 * ny * tokens), BF16),
            pltpu.VMEM((recv_slots, n, group, width), BF16),
            pltpu.VMEM((nz, n, group, width), BF16),
            pltpu.VMEM((n, ny, rows, width), BF16),
            pltpu.VMEM((group, width), F32),
            pltpu.VMEM((rows, rows), F32),
            pltpu.VMEM((nt, rows, rows), BF16),
            pltpu.VMEM((1, rows), F32),
            dma((n,)),
            dma((2 * ny, nz, nt)),
            dma,
            dma((2, max(ny - 1, 1))),
            dma((recv_slots, n)),
            dma((n,)),
            dma,
            dma,
            dma((max(ny - 1, 1),)),
            dma,
            dma((max(ny - 1, 1),)),
            dma((2, ny)),
            dma((max(nt // 2 - 1, 1),)),
            dma((2, nt // 2)),
            dma((nz,)),
            dma((max(nt - 1, 1),)),
            dma((nt,)),
        ],
        compiler_params=pltpu.CompilerParams(
            collective_id=0, has_side_effects=True, vmem_limit_bytes=48 * 1024 * 1024
        ),
        name="normuon",
    )(
        *(
            pltpu.with_memory_space_constraint(v, pltpu.HBM)
            for v in (out_grad, hidden, momentum, second.reshape(1, rows))
        )
    )
    update, momentum_out, second_out = pl.pallas_call(
        write_kernel,
        out_shape=(
            jax.ShapeDtypeStruct((rows, cols), BF16),
            jax.ShapeDtypeStruct((rows, cols), F32),
            jax.ShapeDtypeStruct((1, rows), F32),
        ),
        in_specs=[vmem] * 4,
        out_specs=(anywhere, anywhere, vmem),
        scratch_shapes=[pltpu.VMEM((rows, cols), BF16), dma, dma((2,))],
        compiler_params=pltpu.CompilerParams(vmem_limit_bytes=16 * 1024 * 1024),
        name="write_results",
    )(panel, mom, final, second_out)
    return update, momentum_out, second_out.reshape(rows)


def solution(mesh):
    nz, ny = line_split(mesh.shape["dp"])
    placed = (P("dp", None), P("dp", "tensor"), P("dp", "tensor"), P("dp"))
    return jax.shard_map(
        functools.partial(body, nz, ny, mesh.shape["tensor"]),
        mesh=mesh,
        in_specs=placed,
        out_specs=(P("dp", "tensor"), P("dp", "tensor"), P("dp")),
        check_vma=False,
    )
```

```python
import functools

import jax
import jax.numpy as jnp
from jax import lax
from jax.experimental import pallas as pl
from jax.experimental.pallas import tpu as pltpu
from jax.sharding import PartitionSpec as P

ITERS = 3
quintic_a = 3.4445
quintic_b = -4.775
quintic_c = 2.0315
beta_one = 0.95
beta_two = 0.95

MESH = pl.DeviceIdType.MESH
F32 = jnp.float32
BF16 = jnp.bfloat16


def line_split(n_dp):
    ny = 1
    while ny * ny * 4 <= n_dp and n_dp % (ny * 2) == 0:
        ny *= 2
    return n_dp // ny, ny


def small_dot(a, b):
    return jnp.dot(a.astype(BF16), b.astype(BF16), preferred_element_type=F32)


def kernel(
    nz, ny, nt, n, ff,
    og_hbm, h_hbm, mom_hbm, sec_hbm,
    x, mom, final_ref, secout_ref,
    h, ograw, og_t, recv, send, fin, acc, kept, cross, gram, g_all, sec_ref,
    h_sem, og_sem, og_own, ogy_send, recv_sem, cross_sem, fin_sem, mom_sem, sec_sem,
    hy_send, end_send, fwd_send, og_send, ogx_send, ogc_send, s_send, g_send, g_recv,
):
    tokens, part = h_hbm.shape[0], h_hbm.shape[1] // ny
    rows, width = x.shape[0], part // n
    group = ny * rows
    tau = tokens // nt
    nx = nt // 2
    slots = 2 * ny
    half = nz // 2
    ahead, end_ahead, lag, late, fin_lag = nz + 1, 1, 1, 9, 2
    d = lax.axis_index("dp")
    t = lax.axis_index("tensor")
    z, y = d // ny, lax.rem(d, ny)
    tx, core = t // 2, lax.rem(t, 2)
    lower = z * 2 < nz
    zm = jnp.where(lower, z, nz - 1 - z)
    toward = jnp.where(lower, 1, -1)
    is_end = zm == 0

    def mirrored(jm):
        return jnp.where(lower, jm, nz - 1 - jm)

    def far_slot(jm):
        return half + jm

    def onward_slot(jm):
        if half == 2:
            return nz - 1 - jm
        return jnp.where(zm == half - 1, nz - 1 - jm, far_slot(jm))

    def at(zz, yy):
        return (zz * ny + yy, t)

    def at_y(k):
        return at(z, lax.rem(y + k, ny))

    def at_t(tt):
        return (d, tt)

    def when(cond, fn):
        if isinstance(cond, bool):
            if cond:
                fn()
        else:
            pl.when(cond)(fn)

    def remote(src, dst, send_sem, recv_sem, device):
        pltpu.make_async_remote_copy(
            src, dst, send_sem, recv_sem, device_id=device, device_id_type=MESH
        ).start()

    def arrived(ref, sem):
        pltpu.make_async_copy(ref, ref, sem).wait()

    def block(i, size):
        return pl.ds(pl.multiple_of(i * size, size), size)

    def columns(p, c):
        return block(p * n + c, width)

    inner_z = 1 if half == 2 else zm
    direct = half == 2
    tail = kept.shape[0]
    streamed = n - tail if direct else n
    z_end = jnp.where(lower, 0, nz - 1)

    barrier = pltpu.get_barrier_semaphore()

    def hello(device):
        pl.semaphore_signal(barrier, inc=1, device_id=device, device_id_type=MESH)

    for k in range(1, ny):
        hello(at_y(k))
    for k in range(1, nt):
        hello(at_t(lax.rem(t + k, nt)))

    @pl.when(is_end)
    def _():
        for k in range(ny):
            hello(at(z + toward, k))
            if direct:
                hello(at(z + 2 * toward, k))

    @pl.when(jnp.logical_not(is_end))
    def _():
        if direct:
            for k in range(ny):
                hello(at(z + toward, k))
                hello(at(z + 2 * toward, k))
        else:
            hello(at(z + toward, y))

        def ends():
            for k in range(ny):
                hello(at(z_end, k))

        def next_in():
            hello(at(z - toward, y))

        if half == 2:
            ends()
        else:
            pl.when(zm == 1)(ends)
            pl.when(zm > 1)(next_in)

    greeted = (ny - 1) + (nt - 1)
    pl.semaphore_wait(
        barrier,
        greeted
        + (
            jnp.where(is_end, 2 * ny, 3 * ny) if direct
            else jnp.where(zm == 0, ny, 0) + jnp.where(zm == 1, ny + 1, 0) + jnp.where(zm > 1, 2, 0)
        ),
    )

    def share(i, tt):
        if i == 0:
            return block(lax.rem(tt, 2), tokens // 2)
        return block(tt, tau)

    def rows_of(j):
        return block(j, group)

    def y_send(c):
        for k in range(1, ny):
            p = lax.rem(y + k, ny)
            remote(
                h_hbm.at[:, columns(p, c)], h.at[c, block(y, tokens)],
                hy_send.at[k - 1], h_sem.at[c], at_y(k),
            )

    def mom_load():
        pltpu.make_async_copy(mom_hbm, mom, mom_sem).start()
        pltpu.make_async_copy(sec_hbm, sec_ref, sec_sem).start()

    def process(q, grad):
        cols = block(q, width)
        momentum_out = beta_one * mom[:, cols] + grad
        mom[:, cols] = momentum_out
        panel = (grad + beta_one * momentum_out).astype(BF16)
        x[:, cols] = panel
        gram[...] += lax.dot_general(
            panel, panel, (((1,), (1,)), ((), ())), preferred_element_type=F32
        )

    def process_fin(count, c):
        arrived(fin.at[c, pl.ds(0, count)], fin_sem.at[c])
        for k in range(ny - count, ny):
            p = lax.rem(y + k, ny)
            process(p * n + c, fin[c, p].astype(F32))

    def process_last(count, i):
        arrived(fin.at[streamed + i, pl.ds(0, count)], fin_sem.at[streamed + i])
        for k in range(ny - count, ny):
            p = lax.rem(y + k, ny)
            arrived(cross.at[i, p], cross_sem.at[i, p])
            process(p * n + streamed + i, fin[streamed + i, p].astype(F32) + cross[i, p].astype(F32))

    @pl.when(is_end)
    def _():
        z_in = z + toward

        def og_to_inner(i):
            j = mirrored(nz - 1 - i)
            remote(
                og_hbm.at[share(i, t), rows_of(j)], ograw.at[ny + y, share(i, t), rows_of(j)],
                og_send.at[min(i, 1), 0], og_sem.at[ny + y, j, t], at(z_in, y),
            )

        def own_to_inner(c):
            remote(
                h_hbm.at[:, columns(y, c)], h.at[c, block(ny + y, tokens)],
                end_send, h_sem.at[c], at(z_in, y),
            )

        og_to_inner(0)
        for c in range(min(2, n)):
            y_send(c)
        for i in range(1, nz - 2):
            og_to_inner(i)
        for c in range(min(end_ahead, n)):
            own_to_inner(c)

        def rest(c, carry):
            y_send(c)
            return carry

        lax.fori_loop(min(2, n), n, rest, 0)
        mom_load()
        gram[...] = jnp.zeros_like(gram)

        def forward(c, carry):
            arrived(h.at[c, pl.ds(0, (ny - 1) * tokens)], h_sem.at[c])
            for k in range(1, ny):
                p = lax.rem(y + k, ny)
                remote(
                    h.at[c, block(p, tokens)], h.at[c, block(ny + p, tokens)],
                    fwd_send.at[k - 1], h_sem.at[c], at(z_in, y),
                )

            @pl.when(c + end_ahead < n)
            def _():
                own_to_inner(c + end_ahead)

            @pl.when(c == min(late - 4, n) - 1)
            def _():
                for i in range(nz - 2, nz):
                    og_to_inner(i)

            return carry

        lax.fori_loop(0, n, forward, 0)
        pltpu.make_async_copy(mom_hbm, mom, mom_sem).wait()
        pltpu.make_async_copy(sec_hbm, sec_ref, sec_sem).wait()

        def finish(c, carry):
            process_fin(ny, c)
            return carry

        lax.fori_loop(0, streamed, finish, 0)
        if direct:
            for i in range(tail):
                process_last(ny, i)

    @pl.when(jnp.logical_not(is_end))
    def _():
        near_end = inner_z == 1
        def og_to_peers(i):
            j = mirrored(nz - 1 - i)
            for k in range(1, ny):
                remote(
                    og_hbm.at[share(i, t), rows_of(j)], ograw.at[y, share(i, t), rows_of(j)],
                    og_send.at[min(i, 1), k], og_sem.at[y, j, t], at_y(k),
                )

        og_to_peers(0)
        y_send(0)
        for i in range(1, nz - 2):
            og_to_peers(i)
        pltpu.make_async_copy(og_hbm, ograw.at[y], og_own).start()

        def own_load(c, carry):
            pltpu.make_async_copy(
                h_hbm.at[:, columns(y, c)], h.at[c, block(y, tokens)], h_sem.at[c]
            ).start()
            return carry

        lax.fori_loop(0, n, own_load, 0)
        mom_load()
        gram[...] = jnp.zeros_like(gram)
        if half > 2:
            @pl.when(zm > 1)
            def _():
                h[:, ny * tokens :] = jnp.zeros((n, ny * tokens, width), BF16)
                ograw[ny:] = jnp.zeros((ny,) + ograw.shape[1:], BF16)

        pltpu.make_async_copy(og_hbm, ograw.at[y], og_own).wait()

        def peer_slots(fn):
            for k in range(1, ny):
                fn(lax.rem(y + k, ny))

            def from_end():
                for k in range(1, ny):
                    fn(ny + lax.rem(y + k, ny))

            when(near_end, from_end)

        def each_slot(fn):
            peer_slots(fn)
            when(near_end, functools.partial(fn, ny + y))

        def og_piece(i, slot, tt):
            return ograw.at[slot, share(i, tt), rows_of(mirrored(nz - 1 - i))]

        def to_core(i, slot, tt, k):
            remote(
                og_piece(i, slot, tt), og_piece(i, slot, tt), ogc_send.at[min(i, 1), k],
                og_sem.at[slot, mirrored(nz - 1 - i), tt], at_t(tx * 2 + 1 - core),
            )

        def og_took(i, slot, tt):
            arrived(og_piece(i, slot, tt), og_sem.at[slot, mirrored(nz - 1 - i), tt])

        def share_out(i, slot):
            if i > 0:
                for k in range(1, nx):
                    remote(
                        og_piece(i, slot, t), og_piece(i, slot, t), ogx_send.at[k - 1],
                        og_sem.at[slot, mirrored(nz - 1 - i), t],
                        at_t(lax.rem(tx + k, nx) * 2 + core),
                    )
            to_core(i, slot, t, 0)

        def stage_end(i):
            def go():
                og_took(i, ny + y, t)
                for k in range(1, ny):
                    remote(
                        og_piece(i, ny + y, t), og_piece(i, ny + y, t), ogy_send.at[min(i, 1), k - 1],
                        og_sem.at[ny + y, mirrored(nz - 1 - i), t], at_y(k),
                    )
                share_out(i, ny + y)

            when(near_end, go)

        def stage_a(i):
            def one(slot):
                og_took(i, slot, t)
                share_out(i, slot)

            peer_slots(one)

        def stage_b(i):
            def one(slot):
                for k in range(1, nx):
                    tt = lax.rem(tx + k, nx) * 2 + core
                    og_took(i, slot, tt)
                    to_core(i, slot, tt, k)

            if i > 0:
                each_slot(one)

        def stage_c(i):
            j = mirrored(nz - 1 - i)

            def one(slot):
                if i == 0:
                    og_took(i, slot, tx * 2 + 1 - core)
                else:
                    for k in range(nx):
                        og_took(i, slot, k * 2 + 1 - core)

            each_slot(one)
            for slot in range(slots if half == 2 else 0):
                for r in range(ny):
                    og_t[j, r * rows : (r + 1) * rows, slot * tokens : (slot + 1) * tokens] = (
                        ograw[slot, :, block(j * ny + r, rows)].T
                    )

        def partial(j, c):
            if half > 2:
                total = None
                for slot in range(slots):
                    term = lax.dot_general(
                        ograw[slot, :, rows_of(j)], h[c, slot * tokens : (slot + 1) * tokens],
                        (((0,), (0,)), ((), ())), preferred_element_type=F32,
                    )
                    total = term if total is None else total + term
                return total
            return jnp.dot(og_t[j], h[c], preferred_element_type=F32)

        def took(idx, c):
            arrived(recv.at[idx, c], recv_sem.at[idx, c])

        steps = n + max((nz - 3) * lag, late) + fin_lag

        def step(s, carry):
            first = s - (inner_z - 1) * lag

            @pl.when(s == 0)
            def _():
                for i in range(nz - 2):
                    stage_end(i)
                if 1 < min(ahead, n):
                    y_send(1)
                for i in range(nz - 2, nz):
                    og_to_peers(i)
                for c in range(2, min(ahead, n)):
                    y_send(c)
                for i in range(nz - 2):
                    stage_a(i)
                stage_c(0)

            @pl.when(jnp.logical_and(first >= 0, first < n))
            def _():
                def took_hidden(count):
                    arrived(h.at[first, pl.ds(0, count * tokens)], h_sem.at[first])

                if half == 2:
                    took_hidden(slots)
                else:
                    pl.when(zm == 1)(functools.partial(took_hidden, slots))
                    pl.when(zm > 1)(functools.partial(took_hidden, ny))

                @pl.when(first + ahead < n)
                def _():
                    y_send(first + ahead)

            def far(jm, f):
                j = mirrored(jm)
                own = partial(j, f)
                if half == 2:
                    send[j, f] = own.astype(BF16)
                else:
                    @pl.when(zm == 1)
                    def _():
                        send[j, f] = own.astype(BF16)

                    @pl.when(zm > 1)
                    def _():
                        took(far_slot(jm), f)
                        send[j, f] = (own + recv[far_slot(jm), f].astype(F32)).astype(BF16)

                def onward():
                    remote(
                        send.at[j, f], recv.at[onward_slot(jm), f],
                        s_send.at[j], recv_sem.at[onward_slot(jm), f], at(z + toward, y),
                    )

                if not direct:
                    onward()
                    return
                pl.when(f < streamed)(onward)

                @pl.when(f >= streamed)
                def _():
                    for p in range(ny):
                        remote(
                            send.at[j, f, pl.ds(p * rows, rows)], cross.at[f - streamed, y],
                            s_send.at[j], cross_sem.at[f - streamed, y], at(j, p),
                        )

            @pl.when(jnp.logical_and(first >= 0, first < n))
            def _():
                far(nz - 1, first)


            @pl.when(s == 1)
            def _():
                for i in range(1, nz - 2):
                    stage_b(i)
                    stage_c(i)

            def done_later(v):
                return jnp.clip(jnp.where(v < 2, v, v + 1), 0, n)

            def later(f, carry):
                for jm in range(nz - 2, 1, -1):
                    if jm >= half:
                        far(jm, f)
                    else:
                        pl.when(jm > zm)(functools.partial(far, jm, f))
                return carry

            lax.fori_loop(done_later(first - 1), done_later(first), later, 0)

            @pl.when(s == late - 5)
            def _():
                for i in range(nz - 2, nz):
                    stage_end(i)

            @pl.when(s == late - 4)
            def _():
                for i in range(nz - 2, nz):
                    stage_a(i)

            @pl.when(s == late - 3)
            def _():
                for i in range(nz - 2, nz):
                    stage_b(i)

            @pl.when(s == late - 1)
            def _():
                for i in range(nz - 2, nz):
                    stage_c(i)
                pltpu.make_async_copy(mom_hbm, mom, mom_sem).wait()
                pltpu.make_async_copy(sec_hbm, sec_ref, sec_sem).wait()

            near_lag = (nz - 2 - inner_z) * lag

            def to_end(j, c):
                for k in range(ny):
                    p = lax.rem(y + 1 + k, ny)
                    remote(
                        send.at[j, c, block(p, rows)], fin.at[c, y],
                        s_send.at[j], fin_sem.at[c], at(z_end, p),
                    )

            def to_peers(c):
                for k in range(1, ny):
                    p = lax.rem(y + k, ny)
                    send[z, c, block(p, rows)] = acc[block(p, rows)].astype(BF16)
                    remote(
                        send.at[z, c, block(p, rows)], fin.at[c, y],
                        s_send.at[z], fin_sem.at[c], at_y(k),
                    )

            if direct:
                own = s - max(late - streamed, 0)

                @pl.when(jnp.logical_and(own >= streamed, own < n))
                def _():
                    send[z_end, own] = partial(z_end, own).astype(BF16)
                    to_end(z_end, own)
                    acc[...] = partial(z, own)
                    to_peers(own)
                    kept[own - streamed] = acc[block(y, rows)]


            def done_near(v):
                return jnp.clip(jnp.minimum(2 * (v + 1 - late), v + 1 - near_lag), 0, streamed)

            def near_chunk(c, carry):
                def near(jm):
                    j = mirrored(jm)
                    own = partial(j, c)
                    took(jm, c)
                    send[j, c] = (own + recv[jm, c].astype(F32)).astype(BF16)

                    def onward():
                        remote(
                            send.at[j, c], recv.at[jm, c],
                            s_send.at[j], recv_sem.at[jm, c], at(z - toward, y),
                        )

                    if jm > 0:
                        onward()
                    else:
                        when(near_end, functools.partial(to_end, j, c))
                        if half > 2:
                            pl.when(zm > 1)(onward)

                for jm in range(half - 1):
                    if jm == 0:
                        near(jm)
                    else:
                        pl.when(jm < zm)(functools.partial(near, jm))

                acc[...] = partial(z, c)
                took(inner_z, c)
                acc[...] += recv[inner_z, c].astype(F32)
                if half > 2:
                    @pl.when(zm > 1)
                    def _():
                        took(far_slot(zm), c)
                        acc[...] += recv[far_slot(zm), c].astype(F32)

                to_peers(c)
                process(y * n + c, acc[block(y, rows)])
                return carry

            def fin_chunk(c, carry):
                process_fin(ny - 1, c)
                return carry

            lax.fori_loop(done_near(s - 1), done_near(s), near_chunk, 0)
            lax.fori_loop(done_near(s - 1 - fin_lag), done_near(s - fin_lag), fin_chunk, 0)
            return carry

        lax.fori_loop(0, steps, step, 0)
        if direct:
            for i in range(tail):
                arrived(cross.at[i, y], cross_sem.at[i, y])
                process(y * n + streamed + i, kept[i] + cross[i, y].astype(F32))
                process_last(ny - 1, i)

    g_all[t] = gram[...].astype(BF16)
    for k in range(1, nt):
        pltpu.make_async_remote_copy(
            g_all.at[t], g_all.at[t], g_send.at[k - 1], g_recv.at[t],
            device_id=at_t(lax.rem(t + k, nt)), device_id_type=MESH,
        ).start()
    for k in range(nt):
        @pl.when(k != t)
        def _():
            pltpu.make_async_copy(g_all.at[k], g_all.at[k], g_recv.at[k]).wait()
    summed = g_all[0].astype(F32)
    for k in range(1, nt):
        summed = summed + g_all[k].astype(F32)
    eye = (
        lax.broadcasted_iota(jnp.int32, (rows, rows), 0)
        == lax.broadcasted_iota(jnp.int32, (rows, rows), 1)
    ).astype(F32)
    total = jnp.sum(jnp.sum(summed * eye, axis=0, keepdims=True), axis=1, keepdims=True)
    inverse = 1.0 / (jnp.sqrt(total) + 1e-07)
    current = summed * inverse * inverse
    map_all = None
    for iteration in range(ITERS):
        square = small_dot(current, current)
        map_one = quintic_a * eye + quintic_b * current + quintic_c * square
        map_all = map_one if map_all is None else small_dot(map_one, map_all)
        mapped = small_dot(map_one, current)
        if iteration < ITERS - 1:
            current = small_dot(mapped, map_one)
    energy = jnp.sum(mapped * map_one, axis=0, keepdims=True)
    second_out = beta_two * sec_ref[...] + (1.0 - beta_two) * energy
    secout_ref[...] = second_out
    scale = jnp.sqrt(ff / second_out) * inverse
    final = jnp.sum(eye * scale, axis=1, keepdims=True) * map_all
    final_ref[...] = final

    def sent(ref, sem):
        pltpu.make_async_copy(ref, ref, sem).wait()

    blocks = h.at[:, pl.ds(0, tokens)]

    def og_sent(sems, k):
        sent(ograw.at[0, pl.ds(0, tokens // 2), pl.ds(0, group)], sems.at[0, k])
        sent(ograw.at[0, pl.ds(0, tau), pl.ds(0, (nz - 1) * group)], sems.at[1, k])

    for k in range(1, ny):
        sent(blocks, hy_send.at[k - 1])

    @pl.when(is_end)
    def _():
        og_sent(og_send, 0)
        sent(blocks, end_send)
        for k in range(1, ny):
            sent(blocks, fwd_send.at[k - 1])

    @pl.when(jnp.logical_not(is_end))
    def _():
        def og_forwarded():
            for k in range(1, ny):
                og_sent(ogy_send, k - 1)

        for k in range(1, ny):
            og_sent(og_send, k)
        if half == 2:
            og_forwarded()
        else:
            pl.when(zm == 1)(og_forwarded)

        def og_gather(count):
            pieces = ograw.at[pl.ds(0, count), pl.ds(0, tau), pl.ds(0, (nz - 1) * group)]
            sent(ograw.at[pl.ds(0, count), pl.ds(0, tokens // 2), pl.ds(0, group)], ogc_send.at[0, 0])
            for k in range(1, nx):
                sent(pieces, ogx_send.at[k - 1])
            for k in range(nx):
                sent(pieces, ogc_send.at[1, k])

        if half == 2:
            og_gather(slots - 1)
        else:
            pl.when(zm == 1)(functools.partial(og_gather, slots - 1))
            pl.when(zm > 1)(functools.partial(og_gather, ny - 1))
        for j in range(nz):
            @pl.when(z != j)
            def _():
                sent(send.at[j], s_send.at[j])

        if ny > 1:
            own = send.at[z, :, pl.ds(0, (ny - 1) * rows)]
            sent(own, s_send.at[z])

    for k in range(1, nt):
        sent(g_all.at[0], g_send.at[k - 1])


def write_kernel(x, mom, final_ref, sec_ref, upd_hbm, momout_hbm, secout_ref, out, mom_sem, upd_sem):
    for r in range(4):
        band = pl.ds(r * (mom.shape[0] // 4), mom.shape[0] // 4)
        pltpu.make_async_copy(mom.at[band], momout_hbm.at[band], mom_sem).start()
    high = final_ref[...].astype(BF16)
    secout_ref[...] = sec_ref[...]
    cols = x.shape[1]
    width = 1024 if cols % 1024 == 0 else 512 if cols % 512 == 0 else 128
    n = cols // width

    def finish(c, carry):
        part = pl.ds(pl.multiple_of(c * width, width), width)
        out[:, part] = jnp.dot(high, x[:, part], preferred_element_type=F32).astype(BF16)
        pltpu.make_async_copy(out.at[:, part], upd_hbm.at[:, part], upd_sem.at[0]).start()
        return carry

    lax.fori_loop(0, n, finish, 0)
    pltpu.make_async_copy(mom, momout_hbm, mom_sem).wait()
    pltpu.make_async_copy(out, upd_hbm, upd_sem.at[0]).wait()


def body(nz, ny, nt, out_grad, hidden, momentum, second):
    tokens, cols = hidden.shape
    rows = momentum.shape[0]
    part = cols // ny
    width = 128
    n = part // width
    group = ny * rows
    tail = min(2, n)
    recv_slots = nz // 2 if nz == 4 else nz // 2 + nz
    dma = pltpu.SemaphoreType.DMA
    anywhere = pl.BlockSpec(memory_space=pltpu.HBM)
    vmem = pl.BlockSpec(memory_space=pltpu.VMEM)
    panel, mom, final, second_out = pl.pallas_call(
        functools.partial(kernel, nz, ny, nt, n, float(cols * nt)),
        out_shape=(
            jax.ShapeDtypeStruct((rows, cols), BF16),
            jax.ShapeDtypeStruct((rows, cols), F32),
            jax.ShapeDtypeStruct((rows, rows), F32),
            jax.ShapeDtypeStruct((1, rows), F32),
        ),
        in_specs=[anywhere] * 4,
        out_specs=(vmem, vmem, vmem, vmem),
        scratch_shapes=[
            pltpu.VMEM((n, 2 * ny * tokens, width), BF16),
            pltpu.VMEM((2 * ny, tokens, nz * group), BF16),
            pltpu.VMEM((nz if nz == 4 else 1, group, 2 * ny * tokens), BF16),
            pltpu.VMEM((recv_slots, n, group, width), BF16),
            pltpu.VMEM((nz, n, group, width), BF16),
            pltpu.VMEM((n, ny, rows, width), BF16),
            pltpu.VMEM((group, width), F32),
            pltpu.VMEM((tail, rows, width), F32),
            pltpu.VMEM((tail, ny, rows, width), BF16),
            pltpu.VMEM((rows, rows), F32),
            pltpu.VMEM((nt, rows, rows), BF16),
            pltpu.VMEM((1, rows), F32),
            dma((n,)),
            dma((2 * ny, nz, nt)),
            dma,
            dma((2, max(ny - 1, 1))),
            dma((recv_slots, n)),
            dma((tail, ny)),
            dma((n,)),
            dma,
            dma,
            dma((max(ny - 1, 1),)),
            dma,
            dma((max(ny - 1, 1),)),
            dma((2, ny)),
            dma((max(nt // 2 - 1, 1),)),
            dma((2, nt // 2)),
            dma((nz,)),
            dma((max(nt - 1, 1),)),
            dma((nt,)),
        ],
        compiler_params=pltpu.CompilerParams(
            collective_id=0, has_side_effects=True, vmem_limit_bytes=48 * 1024 * 1024
        ),
        name="normuon",
    )(
        *(
            pltpu.with_memory_space_constraint(v, pltpu.HBM)
            for v in (out_grad, hidden, momentum, second.reshape(1, rows))
        )
    )
    update, momentum_out, second_out = pl.pallas_call(
        write_kernel,
        out_shape=(
            jax.ShapeDtypeStruct((rows, cols), BF16),
            jax.ShapeDtypeStruct((rows, cols), F32),
            jax.ShapeDtypeStruct((1, rows), F32),
        ),
        in_specs=[vmem] * 4,
        out_specs=(anywhere, anywhere, vmem),
        scratch_shapes=[pltpu.VMEM((rows, cols), BF16), dma, dma((2,))],
        compiler_params=pltpu.CompilerParams(vmem_limit_bytes=16 * 1024 * 1024),
        name="write_results",
    )(panel, mom, final, second_out)
    return update, momentum_out, second_out.reshape(rows)


def solution(mesh):
    nz, ny = line_split(mesh.shape["dp"])
    placed = (P("dp", None), P("dp", "tensor"), P("dp", "tensor"), P("dp"))
    return jax.shard_map(
        functools.partial(body, nz, ny, mesh.shape["tensor"]),
        mesh=mesh,
        in_specs=placed,
        out_specs=(P("dp", "tensor"), P("dp", "tensor"), P("dp")),
        check_vma=False,
    )
```

```python
import functools

import jax
import jax.numpy as jnp
from jax import lax
from jax.experimental import pallas as pl
from jax.experimental.pallas import tpu as pltpu
from jax.sharding import PartitionSpec as P

ITERS = 3
quintic_a = 3.4445
quintic_b = -4.775
quintic_c = 2.0315
beta_one = 0.95
beta_two = 0.95

MESH = pl.DeviceIdType.MESH
F32 = jnp.float32
BF16 = jnp.bfloat16


def line_split(n_dp):
    ny = 1
    while ny * ny * 4 <= n_dp and n_dp % (ny * 2) == 0:
        ny *= 2
    return n_dp // ny, ny


def small_dot(a, b):
    return jnp.dot(a.astype(BF16), b.astype(BF16), preferred_element_type=F32)


def kernel(
    nz, ny, nt, n, ff,
    og_hbm, h_hbm, mom_hbm, sec_hbm,
    x, mom, final_ref, secout_ref,
    h, ograw, og_t, recv, send, fin, acc, kept, cross, gram, g_all, sec_ref,
    h_sem, og_sem, og_own, ogy_send, recv_sem, cross_sem, fin_sem, mom_sem, sec_sem,
    hy_send, end_send, fwd_send, og_send, ogx_send, ogc_send, s_send, g_send, g_recv,
):
    tokens, part = h_hbm.shape[0], h_hbm.shape[1] // ny
    rows, width = x.shape[0], part // n
    group = ny * rows
    tau = tokens // nt
    nx = nt // 2
    slots = 2 * ny
    half = nz // 2
    ahead, end_ahead, lag, late, fin_lag = nz + 1, 1, 1, 9, 2
    d = lax.axis_index("dp")
    t = lax.axis_index("tensor")
    z, y = d // ny, lax.rem(d, ny)
    tx, core = t // 2, lax.rem(t, 2)
    lower = z * 2 < nz
    zm = jnp.where(lower, z, nz - 1 - z)
    toward = jnp.where(lower, 1, -1)
    is_end = zm == 0

    def mirrored(jm):
        return jnp.where(lower, jm, nz - 1 - jm)

    def far_slot(jm):
        return half + jm

    def onward_slot(jm):
        if half == 2:
            return nz - 1 - jm
        return jnp.where(zm == half - 1, nz - 1 - jm, far_slot(jm))

    def at(zz, yy):
        return (zz * ny + yy, t)

    def at_y(k):
        return at(z, lax.rem(y + k, ny))

    def at_t(tt):
        return (d, tt)

    def when(cond, fn):
        if isinstance(cond, bool):
            if cond:
                fn()
        else:
            pl.when(cond)(fn)

    def remote(src, dst, send_sem, recv_sem, device):
        pltpu.make_async_remote_copy(
            src, dst, send_sem, recv_sem, device_id=device, device_id_type=MESH
        ).start()

    def arrived(ref, sem):
        pltpu.make_async_copy(ref, ref, sem).wait()

    def block(i, size):
        return pl.ds(pl.multiple_of(i * size, size), size)

    def columns(p, c):
        return block(p * n + c, width)

    inner_z = 1 if half == 2 else zm
    direct = half == 2
    tail = kept.shape[0]
    streamed = n - tail if direct else n
    z_end = jnp.where(lower, 0, nz - 1)

    barrier = pltpu.get_barrier_semaphore()

    def hello(device):
        pl.semaphore_signal(barrier, inc=1, device_id=device, device_id_type=MESH)

    for k in range(1, ny):
        hello(at_y(k))
    for k in range(1, nt):
        hello(at_t(lax.rem(t + k, nt)))

    @pl.when(is_end)
    def _():
        for k in range(ny):
            hello(at(z + toward, k))
            if direct:
                hello(at(z + 2 * toward, k))

    @pl.when(jnp.logical_not(is_end))
    def _():
        if direct:
            for k in range(ny):
                hello(at(z + toward, k))
                hello(at(z + 2 * toward, k))
        else:
            hello(at(z + toward, y))

        def ends():
            for k in range(ny):
                hello(at(z_end, k))

        def next_in():
            hello(at(z - toward, y))

        if half == 2:
            ends()
        else:
            pl.when(zm == 1)(ends)
            pl.when(zm > 1)(next_in)

    greeted = (ny - 1) + (nt - 1)
    pl.semaphore_wait(
        barrier,
        greeted
        + (
            jnp.where(is_end, 2 * ny, 3 * ny) if direct
            else jnp.where(zm == 0, ny, 0) + jnp.where(zm == 1, ny + 1, 0) + jnp.where(zm > 1, 2, 0)
        ),
    )

    def share(i, tt):
        if i == 0:
            return block(lax.rem(tt, 2), tokens // 2)
        return block(tt, tau)

    def rows_of(j):
        return block(j, group)

    def y_send(c):
        for k in range(1, ny):
            p = lax.rem(y + k, ny)
            remote(
                h_hbm.at[:, columns(p, c)], h.at[c, block(y, tokens)],
                hy_send.at[k - 1], h_sem.at[c], at_y(k),
            )

    def mom_load():
        pltpu.make_async_copy(mom_hbm, mom, mom_sem).start()
        pltpu.make_async_copy(sec_hbm, sec_ref, sec_sem).start()

    def process(q, grad):
        cols = block(q, width)
        momentum_out = beta_one * mom[:, cols] + grad
        mom[:, cols] = momentum_out
        panel = (grad + beta_one * momentum_out).astype(BF16)
        x[:, cols] = panel
        gram[...] += lax.dot_general(
            panel, panel, (((1,), (1,)), ((), ())), preferred_element_type=F32
        )

    def process_fin(count, c):
        arrived(fin.at[c, pl.ds(0, count)], fin_sem.at[c])
        for k in range(ny - count, ny):
            p = lax.rem(y + k, ny)
            process(p * n + c, fin[c, p].astype(F32))

    def process_last(count, i):
        arrived(fin.at[streamed + i, pl.ds(0, count)], fin_sem.at[streamed + i])
        for k in range(ny - count, ny):
            p = lax.rem(y + k, ny)
            arrived(cross.at[i, p], cross_sem.at[i, p])
            process(p * n + streamed + i, fin[streamed + i, p].astype(F32) + cross[i, p].astype(F32))

    @pl.when(is_end)
    def _():
        z_in = z + toward

        def og_to_inner(i):
            j = mirrored(nz - 1 - i)
            remote(
                og_hbm.at[share(i, t), rows_of(j)], ograw.at[ny + y, share(i, t), rows_of(j)],
                og_send.at[min(i, 1), 0], og_sem.at[i, ny + y], at(z_in, y),
            )

        def own_to_inner(c):
            remote(
                h_hbm.at[:, columns(y, c)], h.at[c, block(ny + y, tokens)],
                end_send, h_sem.at[c], at(z_in, y),
            )

        og_to_inner(0)
        for c in range(min(2, n)):
            y_send(c)
        for i in range(1, nz - 2):
            og_to_inner(i)
        for c in range(min(end_ahead, n)):
            own_to_inner(c)

        def rest(c, carry):
            y_send(c)
            return carry

        lax.fori_loop(min(2, n), n, rest, 0)
        mom_load()
        gram[...] = jnp.zeros_like(gram)

        def forward(c, carry):
            arrived(h.at[c, pl.ds(0, (ny - 1) * tokens)], h_sem.at[c])
            for k in range(1, ny):
                p = lax.rem(y + k, ny)
                remote(
                    h.at[c, block(p, tokens)], h.at[c, block(ny + p, tokens)],
                    fwd_send.at[k - 1], h_sem.at[c], at(z_in, y),
                )

            @pl.when(c + end_ahead < n)
            def _():
                own_to_inner(c + end_ahead)

            @pl.when(c == min(late - 4, n) - 1)
            def _():
                for i in range(nz - 2, nz):
                    og_to_inner(i)

            return carry

        lax.fori_loop(0, n, forward, 0)
        pltpu.make_async_copy(mom_hbm, mom, mom_sem).wait()
        pltpu.make_async_copy(sec_hbm, sec_ref, sec_sem).wait()

        def finish(c, carry):
            process_fin(ny, c)
            return carry

        lax.fori_loop(0, streamed, finish, 0)
        if direct:
            for i in range(tail):
                process_last(ny, i)

    @pl.when(jnp.logical_not(is_end))
    def _():
        near_end = inner_z == 1
        def og_to_peers(i):
            j = mirrored(nz - 1 - i)
            for k in range(1, ny):
                remote(
                    og_hbm.at[share(i, t), rows_of(j)], ograw.at[y, share(i, t), rows_of(j)],
                    og_send.at[min(i, 1), k], og_sem.at[i, y], at_y(k),
                )

        og_to_peers(0)
        y_send(0)
        for i in range(1, nz - 2):
            og_to_peers(i)
        pltpu.make_async_copy(og_hbm, ograw.at[y], og_own).start()

        def own_load(c, carry):
            pltpu.make_async_copy(
                h_hbm.at[:, columns(y, c)], h.at[c, block(y, tokens)], h_sem.at[c]
            ).start()
            return carry

        lax.fori_loop(0, n, own_load, 0)
        mom_load()
        gram[...] = jnp.zeros_like(gram)
        if half > 2:
            @pl.when(zm > 1)
            def _():
                h[:, ny * tokens :] = jnp.zeros((n, ny * tokens, width), BF16)
                ograw[ny:] = jnp.zeros((ny,) + ograw.shape[1:], BF16)

        pltpu.make_async_copy(og_hbm, ograw.at[y], og_own).wait()

        def peer_slots(fn):
            for k in range(1, ny):
                fn(lax.rem(y + k, ny))

            def from_end():
                for k in range(1, ny):
                    fn(ny + lax.rem(y + k, ny))

            when(near_end, from_end)

        def each_slot(fn):
            peer_slots(fn)
            when(near_end, functools.partial(fn, ny + y))

        def og_piece(i, slot, tt):
            return ograw.at[slot, share(i, tt), rows_of(mirrored(nz - 1 - i))]

        def to_core(i, slot, tt, k):
            remote(
                og_piece(i, slot, tt), og_piece(i, slot, tt), ogc_send.at[min(i, 1), k],
                og_sem.at[i, slots + nx], at_t(tx * 2 + 1 - core),
            )

        def og_took(i, slot):
            arrived(og_piece(i, slot, t), og_sem.at[i, slot])

        def og_gathered(i, sem, share_rows):
            def took_all(count):
                arrived(ograw.at[pl.ds(0, count), pl.ds(0, share_rows), pl.ds(0, group)], og_sem.at[i, sem])

            if half == 2:
                took_all(slots - 1)
            else:
                pl.when(zm == 1)(functools.partial(took_all, slots - 1))
                pl.when(zm > 1)(functools.partial(took_all, ny - 1))

        def share_out(i, slot):
            if i > 0:
                for k in range(1, nx):
                    remote(
                        og_piece(i, slot, t), og_piece(i, slot, t), ogx_send.at[k - 1],
                        og_sem.at[i, slots + tx], at_t(lax.rem(tx + k, nx) * 2 + core),
                    )
            to_core(i, slot, t, 0)

        def stage_end(i):
            def go():
                og_took(i, ny + y)
                for k in range(1, ny):
                    remote(
                        og_piece(i, ny + y, t), og_piece(i, ny + y, t), ogy_send.at[min(i, 1), k - 1],
                        og_sem.at[i, ny + y], at_y(k),
                    )
                share_out(i, ny + y)

            when(near_end, go)

        def stage_a(i):
            def one(slot):
                og_took(i, slot)
                share_out(i, slot)

            peer_slots(one)

        def stage_b(i):
            if i == 0:
                return
            for k in range(1, nx):
                ox = lax.rem(tx + k, nx)
                og_gathered(i, slots + ox, tau)
                each_slot(lambda slot: to_core(i, slot, ox * 2 + core, k))

        def stage_c(i):
            j = mirrored(nz - 1 - i)
            og_gathered(i, slots + nx, tokens // 2)
            for slot in range(slots if half == 2 else 0):
                for r in range(ny):
                    og_t[j, r * rows : (r + 1) * rows, slot * tokens : (slot + 1) * tokens] = (
                        ograw[slot, :, block(j * ny + r, rows)].T
                    )

        def partial(j, c):
            if half > 2:
                total = None
                for slot in range(slots):
                    term = lax.dot_general(
                        ograw[slot, :, rows_of(j)], h[c, slot * tokens : (slot + 1) * tokens],
                        (((0,), (0,)), ((), ())), preferred_element_type=F32,
                    )
                    total = term if total is None else total + term
                return total
            return jnp.dot(og_t[j], h[c], preferred_element_type=F32)

        def took(idx, c):
            arrived(recv.at[c, idx], recv_sem.at[idx, c])

        steps = n + max((nz - 3) * lag, late) + fin_lag

        def step(s, carry):
            first = s - (inner_z - 1) * lag

            @pl.when(s == 0)
            def _():
                for i in range(nz - 2):
                    stage_end(i)
                if 1 < min(ahead, n):
                    y_send(1)
                for i in range(nz - 2, nz):
                    og_to_peers(i)
                for c in range(2, min(ahead, n)):
                    y_send(c)
                for i in range(nz - 2):
                    stage_a(i)
                stage_c(0)

            @pl.when(jnp.logical_and(first >= 0, first < n))
            def _():
                def took_hidden(count):
                    arrived(h.at[first, pl.ds(0, count * tokens)], h_sem.at[first])

                if half == 2:
                    took_hidden(slots)
                else:
                    pl.when(zm == 1)(functools.partial(took_hidden, slots))
                    pl.when(zm > 1)(functools.partial(took_hidden, ny))

                @pl.when(first + ahead < n)
                def _():
                    y_send(first + ahead)

            def far(jm, f):
                j = mirrored(jm)
                own = partial(j, f)
                if half == 2:
                    send[j, f] = own.astype(BF16)
                else:
                    @pl.when(zm == 1)
                    def _():
                        send[j, f] = own.astype(BF16)

                    @pl.when(zm > 1)
                    def _():
                        took(far_slot(jm), f)
                        send[j, f] = (own + recv[f, far_slot(jm)].astype(F32)).astype(BF16)

                def onward():
                    remote(
                        send.at[j, f], recv.at[f, onward_slot(jm)],
                        s_send.at[j], recv_sem.at[onward_slot(jm), f], at(z + toward, y),
                    )

                if not direct:
                    onward()
                    return
                pl.when(f < streamed)(onward)

                @pl.when(f >= streamed)
                def _():
                    for p in range(ny):
                        remote(
                            send.at[j, f, pl.ds(p * rows, rows)], cross.at[f - streamed, y],
                            s_send.at[j], cross_sem.at[f - streamed, y], at(j, p),
                        )

            @pl.when(jnp.logical_and(first >= 0, first < (streamed if direct else n)))
            def _():
                far(nz - 1, first)


            @pl.when(s == 1)
            def _():
                for i in range(1, nz - 2):
                    stage_b(i)
                    stage_c(i)

            def done_later(v):
                return jnp.clip(jnp.where(v < 2, v, v + 1), 0, n)

            def later(f, carry):
                for jm in range(nz - 2, 1, -1):
                    if jm >= half:
                        far(jm, f)
                    else:
                        pl.when(jm > zm)(functools.partial(far, jm, f))
                return carry

            lax.fori_loop(done_later(first - 1), done_later(first), later, 0)

            if direct:
                @pl.when(jnp.logical_and(first >= streamed, first < n))
                def _():
                    far(nz - 1, first)

            @pl.when(s == late - 5)
            def _():
                for i in range(nz - 2, nz):
                    stage_end(i)

            @pl.when(s == late - 4)
            def _():
                for i in range(nz - 2, nz):
                    stage_a(i)

            @pl.when(s == late - 3)
            def _():
                for i in range(nz - 2, nz):
                    stage_b(i)

            @pl.when(s == late - 1)
            def _():
                for i in range(nz - 2, nz):
                    stage_c(i)
                pltpu.make_async_copy(mom_hbm, mom, mom_sem).wait()
                pltpu.make_async_copy(sec_hbm, sec_ref, sec_sem).wait()

            near_lag = (nz - 2 - inner_z) * lag

            def to_end(j, c):
                for k in range(ny):
                    p = lax.rem(y + 1 + k, ny)
                    remote(
                        send.at[j, c, block(p, rows)], fin.at[c, y],
                        s_send.at[j], fin_sem.at[c], at(z_end, p),
                    )

            def to_peers(c):
                for k in range(1, ny):
                    p = lax.rem(y + k, ny)
                    send[z, c, block(p, rows)] = acc[block(p, rows)].astype(BF16)
                    remote(
                        send.at[z, c, block(p, rows)], fin.at[c, y],
                        s_send.at[z], fin_sem.at[c], at_y(k),
                    )

            if direct:
                own = s - max(late - streamed, 0)

                @pl.when(jnp.logical_and(own >= streamed, own < n))
                def _():
                    send[z_end, own] = partial(z_end, own).astype(BF16)
                    to_end(z_end, own)
                    acc[...] = partial(z, own)
                    to_peers(own)
                    kept[own - streamed] = acc[block(y, rows)]


            def done_near(v):
                return jnp.clip(jnp.minimum(2 * (v + 1 - late), v + 1 - near_lag), 0, streamed)

            def near_chunk(c, carry):
                def near(jm):
                    j = mirrored(jm)
                    own = partial(j, c)
                    took(jm, c)
                    send[j, c] = (own + recv[c, jm].astype(F32)).astype(BF16)

                    def onward():
                        remote(
                            send.at[j, c], recv.at[c, jm],
                            s_send.at[j], recv_sem.at[jm, c], at(z - toward, y),
                        )

                    if jm > 0:
                        onward()
                    else:
                        when(near_end, functools.partial(to_end, j, c))
                        if half > 2:
                            pl.when(zm > 1)(onward)

                for jm in range(half - 1):
                    if jm == 0:
                        near(jm)
                    else:
                        pl.when(jm < zm)(functools.partial(near, jm))

                acc[...] = partial(z, c)
                took(inner_z, c)
                acc[...] += recv[c, inner_z].astype(F32)
                if half > 2:
                    @pl.when(zm > 1)
                    def _():
                        took(far_slot(zm), c)
                        acc[...] += recv[c, far_slot(zm)].astype(F32)

                to_peers(c)
                process(y * n + c, acc[block(y, rows)])
                return carry

            def fin_chunk(c, carry):
                process_fin(ny - 1, c)
                return carry

            lax.fori_loop(done_near(s - 1), done_near(s), near_chunk, 0)
            lax.fori_loop(done_near(s - 1 - fin_lag), done_near(s - fin_lag), fin_chunk, 0)
            return carry

        lax.fori_loop(0, steps, step, 0)
        if direct:
            for i in range(tail):
                arrived(cross.at[i, y], cross_sem.at[i, y])
                process(y * n + streamed + i, kept[i] + cross[i, y].astype(F32))
                process_last(ny - 1, i)

    g_all[t] = gram[...].astype(BF16)
    for k in range(1, nt):
        pltpu.make_async_remote_copy(
            g_all.at[t], g_all.at[t], g_send.at[k - 1], g_recv.at[t],
            device_id=at_t(lax.rem(t + k, nt)), device_id_type=MESH,
        ).start()
    for k in range(nt):
        @pl.when(k != t)
        def _():
            pltpu.make_async_copy(g_all.at[k], g_all.at[k], g_recv.at[k]).wait()
    summed = g_all[0].astype(F32)
    for k in range(1, nt):
        summed = summed + g_all[k].astype(F32)
    eye = (
        lax.broadcasted_iota(jnp.int32, (rows, rows), 0)
        == lax.broadcasted_iota(jnp.int32, (rows, rows), 1)
    ).astype(F32)
    total = jnp.sum(jnp.sum(summed * eye, axis=0, keepdims=True), axis=1, keepdims=True)
    inverse = 1.0 / (jnp.sqrt(total) + 1e-07)
    current = summed * inverse * inverse
    map_all = None
    for iteration in range(ITERS):
        square = small_dot(current, current)
        map_one = quintic_a * eye + quintic_b * current + quintic_c * square
        map_all = map_one if map_all is None else small_dot(map_one, map_all)
        mapped = small_dot(map_one, current)
        if iteration < ITERS - 1:
            current = small_dot(mapped, map_one)
    energy = jnp.sum(mapped * map_one, axis=0, keepdims=True)
    second_out = beta_two * sec_ref[...] + (1.0 - beta_two) * energy
    secout_ref[...] = second_out
    scale = jnp.sqrt(ff / second_out) * inverse
    final = jnp.sum(eye * scale, axis=1, keepdims=True) * map_all
    final_ref[...] = final

    def sent(ref, sem):
        pltpu.make_async_copy(ref, ref, sem).wait()

    blocks = h.at[:, pl.ds(0, tokens)]

    def og_sent(sems, k):
        sent(ograw.at[0, pl.ds(0, tokens // 2), pl.ds(0, group)], sems.at[0, k])
        sent(ograw.at[0, pl.ds(0, tau), pl.ds(0, (nz - 1) * group)], sems.at[1, k])

    for k in range(1, ny):
        sent(blocks, hy_send.at[k - 1])

    @pl.when(is_end)
    def _():
        og_sent(og_send, 0)
        sent(blocks, end_send)
        for k in range(1, ny):
            sent(blocks, fwd_send.at[k - 1])

    @pl.when(jnp.logical_not(is_end))
    def _():
        def og_forwarded():
            for k in range(1, ny):
                og_sent(ogy_send, k - 1)

        for k in range(1, ny):
            og_sent(og_send, k)
        if half == 2:
            og_forwarded()
        else:
            pl.when(zm == 1)(og_forwarded)

        def og_gather(count):
            pieces = ograw.at[pl.ds(0, count), pl.ds(0, tau), pl.ds(0, (nz - 1) * group)]
            sent(ograw.at[pl.ds(0, count), pl.ds(0, tokens // 2), pl.ds(0, group)], ogc_send.at[0, 0])
            for k in range(1, nx):
                sent(pieces, ogx_send.at[k - 1])
            for k in range(nx):
                sent(pieces, ogc_send.at[1, k])

        if half == 2:
            og_gather(slots - 1)
        else:
            pl.when(zm == 1)(functools.partial(og_gather, slots - 1))
            pl.when(zm > 1)(functools.partial(og_gather, ny - 1))
        for j in range(nz):
            @pl.when(z != j)
            def _():
                sent(send.at[j], s_send.at[j])

        if ny > 1:
            own = send.at[z, :, pl.ds(0, (ny - 1) * rows)]
            sent(own, s_send.at[z])

    for k in range(1, nt):
        sent(g_all.at[0], g_send.at[k - 1])


def write_kernel(x, mom, final_ref, sec_ref, upd_hbm, momout_hbm, secout_ref, out, mom_sem, upd_sem):
    for r in range(4):
        band = pl.ds(r * (mom.shape[0] // 4), mom.shape[0] // 4)
        pltpu.make_async_copy(mom.at[band], momout_hbm.at[band], mom_sem).start()
    high = final_ref[...].astype(BF16)
    secout_ref[...] = sec_ref[...]
    cols = x.shape[1]
    width = 1024 if cols % 1024 == 0 else 512 if cols % 512 == 0 else 128
    n = cols // width

    def finish(c, carry):
        part = pl.ds(pl.multiple_of(c * width, width), width)
        out[:, part] = jnp.dot(high, x[:, part], preferred_element_type=F32).astype(BF16)
        pltpu.make_async_copy(out.at[:, part], upd_hbm.at[:, part], upd_sem.at[0]).start()
        return carry

    lax.fori_loop(0, n, finish, 0)
    pltpu.make_async_copy(mom, momout_hbm, mom_sem).wait()
    pltpu.make_async_copy(out, upd_hbm, upd_sem.at[0]).wait()


def body(nz, ny, nt, out_grad, hidden, momentum, second):
    tokens, cols = hidden.shape
    rows = momentum.shape[0]
    part = cols // ny
    width = 128
    n = part // width
    group = ny * rows
    tail = min(2, n)
    recv_slots = nz // 2 if nz == 4 else nz // 2 + nz
    dma = pltpu.SemaphoreType.DMA
    anywhere = pl.BlockSpec(memory_space=pltpu.HBM)
    vmem = pl.BlockSpec(memory_space=pltpu.VMEM)
    panel, mom, final, second_out = pl.pallas_call(
        functools.partial(kernel, nz, ny, nt, n, float(cols * nt)),
        out_shape=(
            jax.ShapeDtypeStruct((rows, cols), BF16),
            jax.ShapeDtypeStruct((rows, cols), F32),
            jax.ShapeDtypeStruct((rows, rows), F32),
            jax.ShapeDtypeStruct((1, rows), F32),
        ),
        in_specs=[anywhere] * 4,
        out_specs=(vmem, vmem, vmem, vmem),
        scratch_shapes=[
            pltpu.VMEM((n, 2 * ny * tokens, width), BF16),
            pltpu.VMEM((2 * ny, tokens, nz * group), BF16),
            pltpu.VMEM((nz if nz == 4 else 1, group, 2 * ny * tokens), BF16),
            pltpu.VMEM((n, recv_slots, group, width), BF16),
            pltpu.VMEM((nz, n, group, width), BF16),
            pltpu.VMEM((n, ny, rows, width), BF16),
            pltpu.VMEM((group, width), F32),
            pltpu.VMEM((tail, rows, width), F32),
            pltpu.VMEM((tail, ny, rows, width), BF16),
            pltpu.VMEM((rows, rows), F32),
            pltpu.VMEM((nt, rows, rows), BF16),
            pltpu.VMEM((1, rows), F32),
            dma((n,)),
            dma((nz, 2 * ny + nt // 2 + 1)),
            dma,
            dma((2, max(ny - 1, 1))),
            dma((recv_slots, n)),
            dma((tail, ny)),
            dma((n,)),
            dma,
            dma,
            dma((max(ny - 1, 1),)),
            dma,
            dma((max(ny - 1, 1),)),
            dma((2, ny)),
            dma((max(nt // 2 - 1, 1),)),
            dma((2, nt // 2)),
            dma((nz,)),
            dma((max(nt - 1, 1),)),
            dma((nt,)),
        ],
        compiler_params=pltpu.CompilerParams(
            collective_id=0, has_side_effects=True, vmem_limit_bytes=48 * 1024 * 1024
        ),
        name="normuon",
    )(
        *(
            pltpu.with_memory_space_constraint(v, pltpu.HBM)
            for v in (out_grad, hidden, momentum, second.reshape(1, rows))
        )
    )
    update, momentum_out, second_out = pl.pallas_call(
        write_kernel,
        out_shape=(
            jax.ShapeDtypeStruct((rows, cols), BF16),
            jax.ShapeDtypeStruct((rows, cols), F32),
            jax.ShapeDtypeStruct((1, rows), F32),
        ),
        in_specs=[vmem] * 4,
        out_specs=(anywhere, anywhere, vmem),
        scratch_shapes=[pltpu.VMEM((rows, cols), BF16), dma, dma((2,))],
        compiler_params=pltpu.CompilerParams(vmem_limit_bytes=16 * 1024 * 1024),
        name="write_results",
    )(panel, mom, final, second_out)
    return update, momentum_out, second_out.reshape(rows)


def solution(mesh):
    nz, ny = line_split(mesh.shape["dp"])
    placed = (P("dp", None), P("dp", "tensor"), P("dp", "tensor"), P("dp"))
    return jax.shard_map(
        functools.partial(body, nz, ny, mesh.shape["tensor"]),
        mesh=mesh,
        in_specs=placed,
        out_specs=(P("dp", "tensor"), P("dp", "tensor"), P("dp")),
        check_vma=False,
    )
```
